128 devices in a mesh: dp: 4 (over z_hi, core), ctx: 32 (over z_lo, x, y).
Axes of the slice: x: 4, y: 4, z: 4 (z_hi: 2, z_lo: 2; z = z_hi * 2 + z_lo), core: 2. Of those that a mesh axis runs over, the one named last changes fastest.
Arguments:
- tokens: bfloat16 [16384, 1792], P(('dp', 'ctx')), may hold values from -24 to 24
- cotangent: bfloat16 [16384, 1792], P(('dp', 'ctx')), may hold values from -6 to 6
- expert_ids: int32 [16384, 4], P(('dp', 'ctx')), may hold values from 0 to 63, all different within a row; in each aligned block of 128 rows (0 to 127, 128 to 255, ...) at most 10 rows name the same one
- norm_gain: float32 [1792], replicated, may hold values from 0.5 to 1.5
- router_weight: bfloat16 [1792, 64], replicated, may hold values from -0.125 to 0.125
- gate_weight: bfloat16 [64, 1792, 1536], P('ctx', None, 'dp'), may hold values from -0.125 to 0.125
- up_weight: bfloat16 [64, 1792, 1536], P('ctx', None, 'dp'), may hold values from -0.125 to 0.125
- down_weight: bfloat16 [64, 1536, 1792], P('ctx', 'dp'), may hold values from -0.15625 to 0.15625
Outputs:
- grad_tokens: bfloat16 [16384, 1792], P(('dp', 'ctx'))
- grad_gate: bfloat16 [64, 1792, 1536], P('ctx', None, 'dp')
- grad_up: bfloat16 [64, 1792, 1536], P('ctx', None, 'dp')
- grad_down: bfloat16 [64, 1536, 1792], P('ctx', 'dp')
- grad_router: float32 [1792, 64], P(('dp', 'ctx'))
- grad_gain: float32 [1792], P(('dp', 'ctx'))
The draws below stay inside these ranges and needn't reach their ends.
Inputs may be any that keep to these rules, and one draw needn't show every extreme that they name: `expert_ids`: each row names 4 different experts; among the rows of one device no expert is named more than 10 times.
All inputs are finite; a program needn't handle non-finite values.
Results may differ from the reference program's by a relative error of at most 0.02.
Values may be sent and summed in bfloat16 or wider, within the bound.
A program may use at most 192 MiB of HBM per device.

```python
import math
import jax
import jax.numpy as jnp
import numpy as np
from jax import lax

D = 1792
FF = 1536
TOP = 4
TOK_DEV = 128
EXPERTS = 64
CAP = 10
TOKENS = 16384
N_DP = 4
N_CTX = 32


def raised(values, own_key, source, target, blocks, factor):
    def block_of(dim):
        return (jnp.arange(values.shape[dim]) // (values.shape[dim] // blocks)).reshape((-1,) + (1,) * (values.ndim - 1 - dim))

    near = jax.random.permutation(own_key, blocks)[block_of(target)]
    second = (block_of(target) + blocks // 2) % blocks
    return jnp.where((block_of(source) == near) | (block_of(source) == second), factor * values, values)


def block_scale(stream_key, shape, cuts, smallest, largest):
    gain, own = 1.0, jax.random.fold_in(stream_key, 6)
    for axis_at, shards_of in cuts:
        draws = jnp.exp(jax.random.uniform(jax.random.fold_in(own, axis_at), (shards_of,), jnp.float32, smallest / len(cuts), largest / len(cuts)))
        gain = gain * jnp.repeat(draws, shape[axis_at] // shards_of).reshape([-1 if axis == axis_at else 1 for axis in range(len(shape))])
    return gain


def shared_out(key, own, number, rows, count, top, bound, skew):
    order = jax.random.permutation(key, count)
    crowded, common = load_shares(count, rows * top, bound, skew, True), load_shares(count, rows * top, bound, skew, False)
    places = jnp.arange(count)

    def named(lengths, rotation):
        used = int((lengths > 0).sum())
        fixed = max(1, used // 4)
        moved = fixed + (places - fixed + rotation * (used - fixed)) % max(1, count - fixed)
        return jnp.zeros((count,), jnp.int32).at[order[jnp.where(places < fixed, places, moved)]].set(jnp.asarray(lengths, jnp.int32))

    lengths = jnp.where(number % 4 == 0, named(crowded, number // 4), named(common, number - number // 4 - 1))
    mixed = jax.random.permutation(jax.random.fold_in(own, 3), count)
    donor, taker = mixed[0:count // 2 * 2:2], mixed[1:count // 2 * 2:2]
    room = jnp.minimum(lengths[donor] - 1, bound - lengths[taker]) // 2
    room = jnp.where((donor == order[0]) | (taker == order[0]) | (lengths[taker] == 0), 0, jnp.maximum(room, 0))
    moved = jax.random.randint(jax.random.fold_in(own, 4), (count // 2,), 0, 1 << 20) % (room + 1)
    lengths = lengths.at[donor].add(-moved).at[taker].add(moved)
    items = jnp.searchsorted(jnp.cumsum(lengths), jnp.arange(rows * top), side="right").astype(jnp.int32)
    table = items.reshape(top, rows).T
    table = table[jax.random.permutation(jax.random.fold_in(own, 1), rows)]
    rotation = jax.random.randint(jax.random.fold_in(own, 2), (rows, 1), 0, top)
    return jnp.take_along_axis(table, (jnp.arange(top)[None, :] + rotation) % top, axis=1)


def load_shares(number_of, total, limit, lean, full):
    portions = [(1 << 20) // math.isqrt(rank ** lean) + 1 for rank in range(1, number_of + 1)]
    largest = limit if full else min(limit, max(-(-total // number_of), total * portions[0] // sum(portions)))
    least = 1 if total - largest >= number_of - 1 else 0
    counts, spare = [largest] + [least] * (number_of - 1), total - largest - least * (number_of - 1)
    while spare > 0:
        free = [i for i in range(1, number_of) if counts[i] < largest] or [i for i in range(1, number_of) if counts[i] < limit]
        pool, budget = sum([portions[i] for i in free]), spare
        for i in free:
            extra = min(limit - counts[i], max(1, budget * portions[i] // pool), spare)
            counts[i] = counts[i] + extra
            spare = spare - extra
    return np.array(counts)


def bell_draw(own_key, shape, width, most, pieces=(), held_as=jnp.bfloat16):
    gain = block_scale(own_key, shape, pieces, -0.22, 0.18) if pieces else 1.0
    result = jax.random.normal(own_key, shape, jnp.float32) * width * gain
    return jnp.minimum(jnp.maximum(result, -most), most).astype(held_as)


def gaussian_with(stream_key, shape, spread, limit, pieces, heavy, kind=jnp.bfloat16):
    values = spread * jax.random.normal(stream_key, shape, jnp.float32)
    if pieces:
        values = values * block_scale(stream_key, shape, pieces, -0.22, 0.18)
    return jnp.clip(raised(values, jax.random.fold_in(stream_key, 3), *heavy), -limit, limit).astype(kind)


def setup_inputs(seed: int = 0) -> dict:
    keys = jax.random.split(jax.random.key(seed), 9)
    tokens = gaussian_with(keys[0], (TOKENS, D), 1.0, 24.0, ((0, 128),), (0, 1, 128, 5.5))
    cotangent = bell_draw(keys[1], (TOKENS, D), 1.0, 6.0, ((0, 128),))
    expert_ids_keys = jax.random.split(jax.random.fold_in(keys[2], 1), TOKENS // TOK_DEV)
    expert_ids_turns = jax.random.permutation(jax.random.fold_in(keys[2], 3), TOKENS // TOK_DEV)
    expert_ids = jax.vmap(lambda own, number: shared_out(jax.random.fold_in(keys[2], 2), own, number, TOK_DEV, EXPERTS, TOP, CAP, 2))(expert_ids_keys, expert_ids_turns).reshape((TOKENS, TOP))
    norm_gain = jnp.clip(1.0 + 0.1 * jax.random.normal(keys[3], (D,), jnp.float32), 0.5, 1.5)
    router_weight = bell_draw(keys[4], (D, EXPERTS), D ** -0.5, 0.125)
    gate_weight = bell_draw(keys[5], (EXPERTS, D, FF), D ** -0.5, 0.125, ((0, 32), (2, 4)))
    up_weight = bell_draw(keys[6], (EXPERTS, D, FF), D ** -0.5, 0.125, ((0, 32), (2, 4)))
    down_weight = bell_draw(keys[7], (EXPERTS, FF, D), FF ** -0.5, 0.15625, ((0, 32), (1, 4)))
    return dict(tokens=tokens, cotangent=cotangent, expert_ids=expert_ids, norm_gain=norm_gain, router_weight=router_weight, gate_weight=gate_weight, up_weight=up_weight, down_weight=down_weight)


EPSILON = 1e-05
SWISH_SCALE = 1.702

def reference(tokens, cotangent, expert_ids, norm_gain, router_weight, gate_weight, up_weight, down_weight):
    ntoken = tokens.shape[0]
    widened = tokens.astype(jnp.float32)
    inverse = lax.rsqrt(lax.optimization_barrier(jnp.mean(widened * widened, axis=1, keepdims=True)) + EPSILON)
    scaled = widened * inverse
    normed = (scaled * norm_gain).astype(jnp.bfloat16)
    logits = jnp.dot(normed, router_weight, preferred_element_type=jnp.float32)
    chosen = jnp.take_along_axis(logits, expert_ids, axis=1)
    lifted = jnp.exp(chosen)
    gates = lifted / lax.optimization_barrier(jnp.sum(lifted, axis=1, keepdims=True))
    devices = N_DP * N_CTX
    per_device = TOK_DEV * TOP
    block_ids = expert_ids.reshape(devices, per_device)
    labels = jnp.arange(EXPERTS, dtype=jnp.int32)
    hits = (block_ids[:, :, None] == labels).astype(jnp.int32)
    rank = lax.optimization_barrier(jnp.sum((jnp.cumsum(hits, axis=1) - 1) * hits, axis=2))
    position = jnp.arange(devices, dtype=jnp.int32)[:, None] * CAP + rank
    assign = jnp.arange(devices * per_device, dtype=jnp.int32)
    flat_ids = block_ids.reshape(-1)
    flat_pos = position.reshape(-1).astype(jnp.int32)
    table = jnp.zeros((EXPERTS, devices * CAP), jnp.int32).at[flat_ids, flat_pos].set(assign)
    present_all = jnp.zeros((EXPERTS, devices * CAP), jnp.float32).at[flat_ids, flat_pos].set(1.0)
    gates_flat = gates.reshape(-1)

    def expert_step(carry, inputs):
        grad_tok, score_acc = carry
        entry, present, w_gate, w_up, w_down = inputs
        token = entry // TOP
        keep = present[:, None] > 0.0
        rows = jnp.where(keep, normed[token], jnp.zeros_like(normed[token]))
        upstream = jnp.where(keep, cotangent[token], jnp.zeros_like(cotangent[token]))
        weight = present * gates_flat[entry]
        gate_pre = jnp.dot(rows, w_gate, preferred_element_type=jnp.float32)
        up_pre = jnp.dot(rows, w_up, preferred_element_type=jnp.float32)
        squash = jax.nn.sigmoid(SWISH_SCALE * gate_pre)
        hidden = (gate_pre * squash * (up_pre + 1.0)).astype(jnp.bfloat16)
        grad_out = jnp.dot(upstream, w_down.T, preferred_element_type=jnp.float32)
        score = lax.optimization_barrier(jnp.sum(grad_out * hidden.astype(jnp.float32), axis=1))
        grad_hidden = weight[:, None] * grad_out
        slope = squash + SWISH_SCALE * gate_pre * squash * (1.0 - squash)
        grad_pre_gate = (grad_hidden * (up_pre + 1.0) * slope).astype(jnp.bfloat16)
        grad_pre_up = (grad_hidden * gate_pre * squash).astype(jnp.bfloat16)
        scaled_up = (weight[:, None] * upstream.astype(jnp.float32)).astype(jnp.bfloat16)
        down_grad = jnp.dot(hidden.T, scaled_up, preferred_element_type=jnp.float32).astype(jnp.bfloat16)
        gate_grad = jnp.dot(rows.T, grad_pre_gate, preferred_element_type=jnp.float32).astype(jnp.bfloat16)
        up_grad = jnp.dot(rows.T, grad_pre_up, preferred_element_type=jnp.float32).astype(jnp.bfloat16)
        back = jnp.dot(grad_pre_gate, w_gate.T, preferred_element_type=jnp.float32)
        back = back + jnp.dot(grad_pre_up, w_up.T, preferred_element_type=jnp.float32)
        grad_tok = grad_tok.at[token].add(back)
        score_acc = score_acc.at[entry].add(score * present)
        return ((grad_tok, score_acc), (gate_grad, up_grad, down_grad))
    start = (jnp.zeros((ntoken, D), jnp.float32), jnp.zeros((ntoken * TOP,), jnp.float32))
    (grad_tok, score_acc), (grad_gate, grad_up, grad_down) = lax.scan(expert_step, start, (table, present_all, gate_weight, up_weight, down_weight))
    score_tok = score_acc.reshape(ntoken, TOP)
    mixed = lax.optimization_barrier(jnp.sum(gates * score_tok, axis=1, keepdims=True))
    grad_chosen = gates * (score_tok - mixed)
    member = expert_ids[:, :, None] == labels
    grad_logits = lax.optimization_barrier(jnp.sum(jnp.where(member, grad_chosen[:, :, None], 0.0), axis=1)).astype(jnp.bfloat16)
    grad_normed = grad_tok + jnp.dot(grad_logits, router_weight.T, preferred_element_type=jnp.float32)
    grad_router = jnp.dot(normed.T, grad_logits, preferred_element_type=jnp.float32)
    grad_gain = lax.optimization_barrier(jnp.sum(grad_normed * scaled, axis=0))
    grad_scaled = grad_normed * norm_gain
    correction = lax.optimization_barrier(jnp.mean(grad_scaled * scaled, axis=1, keepdims=True))
    grad_tokens = (cotangent.astype(jnp.float32) + inverse * (grad_scaled - scaled * correction)).astype(jnp.bfloat16)
    return (grad_tokens, grad_gate, grad_up, grad_down, grad_router, grad_gain)
```

```python
import functools

import jax
import jax.numpy as jnp
from jax import lax
from jax.experimental import pallas as pl
from jax.experimental.pallas import tpu as pltpu
from jax.sharding import PartitionSpec as P

EPSILON = 1e-05
SWISH_SCALE = 1.702
MESH = pl.DeviceIdType.MESH
SLOTS = 8
EXTRA = 2
DEVICES = 128


def coordinates():
    dp, ctx = lax.axis_index("dp"), lax.axis_index("ctx")
    return (ctx // 4) % 4, ctx % 4, (dp // 2) * 2 + ctx // 16, dp % 2


def device_of(x, y, z, core):
    return (z // 2) * 2 + core, (z % 2) * 16 + x * 4 + y


def exchange_kernel(count, swaps, keeps, source_block, target_block, *refs):
    sends, refs = refs[:count], refs[count:]
    gives, refs = refs[:swaps], refs[swaps:]
    owns, refs = refs[:keeps], refs[keeps:]
    lands, refs = refs[:count], refs[count:]
    takes, refs = refs[:swaps], refs[swaps:]
    send_sem, recv_sem, local_sem, swap_send, swap_recv = refs
    x, y, z, core = coordinates()
    mine = device_of(x, y, z, core)

    def peer(k):
        return device_of(
            (x + k) % 4,
            (y + k + k // 4) % 4,
            (z + k + k // 16) % 4,
            (core + k // 64 + k // 4) % 2,
        )

    barrier = pltpu.get_barrier_semaphore()

    def greet(k, carry):
        pl.semaphore_signal(barrier, inc=1, device_id=peer(k), device_id_type=MESH)
        return carry

    lax.fori_loop(1, DEVICES, greet, 0)
    pl.semaphore_wait(barrier, DEVICES - 1)

    def copy(i, k, slot):
        dp, ctx = peer(k)
        return pltpu.make_async_remote_copy(
            src_ref=sends[i].at[source_block(dp, ctx)],
            dst_ref=lands[i].at[slot],
            send_sem=send_sem.at[i, k],
            recv_sem=recv_sem.at[i, slot],
            device_id=(dp, ctx),
            device_id_type=MESH,
        )

    partner = device_of(x, y, z, 1 - core)
    swapped = [
        pltpu.make_async_remote_copy(
            src_ref=gives[i],
            dst_ref=takes[i].at[core] if keeps else takes[i],
            send_sem=swap_send.at[i],
            recv_sem=swap_recv.at[i],
            device_id=partner,
            device_id_type=MESH,
        )
        for i in range(swaps)
    ]
    own_slot = target_block(*mine)
    kept = [
        pltpu.make_async_copy(
            sends[i].at[source_block(*mine)], lands[i].at[own_slot], local_sem.at[i]
        )
        for i in range(count)
    ] + [
        pltpu.make_async_copy(owns[i], takes[i].at[core], local_sem.at[count + i])
        for i in range(keeps)
    ]

    def start(k, carry):
        for i in range(count):
            copy(i, k, own_slot).start()
        return carry

    lax.fori_loop(1, DEVICES, start, 0)
    for item in swapped + kept:
        item.start()

    def finish(k, carry):
        slot = target_block(*peer(k))
        for i in range(count):
            copy(i, k, slot).wait()
        return carry

    lax.fori_loop(1, DEVICES, finish, 0)
    for item in swapped + kept:
        item.wait()


def exchange(sends, gives, owns, source_block, target_block, collective_id):
    count, swaps, keeps = len(sends), len(gives), len(owns)
    pair = (2,) if keeps else ()
    anywhere = pl.BlockSpec(memory_space=pl.ANY)
    out = pl.pallas_call(
        functools.partial(exchange_kernel, count, swaps, keeps, source_block, target_block),
        out_shape=[jax.ShapeDtypeStruct((DEVICES,) + a.shape[1:], a.dtype) for a in sends]
        + [jax.ShapeDtypeStruct(pair + a.shape, a.dtype) for a in gives],
        in_specs=[anywhere] * (count + swaps + keeps),
        out_specs=[anywhere] * (count + swaps),
        scratch_shapes=[
            pltpu.SemaphoreType.DMA((count, DEVICES)),
            pltpu.SemaphoreType.DMA((count, DEVICES)),
            pltpu.SemaphoreType.DMA((count + keeps,)),
            pltpu.SemaphoreType.DMA((max(swaps, 1),)),
            pltpu.SemaphoreType.DMA((max(swaps, 1),)),
        ],
        compiler_params=pltpu.CompilerParams(
            collective_id=collective_id, has_side_effects=True
        ),
    )(*sends, *gives, *owns)
    return out[:count], out[count:]


def expert_of(dp, ctx):
    return 2 * ctx + dp % 2


def linear(dp, ctx):
    return dp * 32 + ctx


def half_and_expert(dp, ctx):
    return (dp // 2) * 64 + expert_of(dp, ctx)


def expert_pass(rows, upstream, gate_halves, up_halves, down_halves):
    parts, back, score = [], None, None
    for w_gate, w_up, w_down in zip(gate_halves, up_halves, down_halves):
        gate_pre = jnp.dot(rows, w_gate, preferred_element_type=jnp.float32)
        up_pre = jnp.dot(rows, w_up, preferred_element_type=jnp.float32)
        squash = jax.nn.sigmoid(SWISH_SCALE * gate_pre)
        hidden = (gate_pre * squash * (up_pre + 1.0)).astype(jnp.bfloat16)
        grad_hidden = jnp.einsum("rd,fd->rf", upstream, w_down, preferred_element_type=jnp.float32)
        here = jnp.sum(grad_hidden * hidden.astype(jnp.float32), axis=1)
        slope = squash + SWISH_SCALE * gate_pre * squash * (1.0 - squash)
        pre_gate = (grad_hidden * (up_pre + 1.0) * slope).astype(jnp.bfloat16)
        pre_up = (grad_hidden * gate_pre * squash).astype(jnp.bfloat16)
        down_grad = jnp.einsum(
            "rf,rd->fd", hidden, upstream, preferred_element_type=jnp.float32
        ).astype(jnp.bfloat16)
        gate_grad = jnp.einsum(
            "rd,rf->df", rows, pre_gate, preferred_element_type=jnp.float32
        ).astype(jnp.bfloat16)
        up_grad = jnp.einsum(
            "rd,rf->df", rows, pre_up, preferred_element_type=jnp.float32
        ).astype(jnp.bfloat16)
        part = jnp.einsum("rf,df->rd", pre_gate, w_gate, preferred_element_type=jnp.float32)
        part = part + jnp.einsum("rf,df->rd", pre_up, w_up, preferred_element_type=jnp.float32)
        back = part if back is None else back + part
        score = here if score is None else score + here
        parts.append((gate_grad, up_grad, down_grad))
    return parts, back, score


def body(
    tokens, cotangent, expert_ids, norm_gain, router_weight, gate_weight, up_weight, down_weight
):
    experts = router_weight.shape[1]
    rows_here, width = tokens.shape
    core = lax.axis_index("dp") % 2
    widened = tokens.astype(jnp.float32)
    inverse = lax.rsqrt(jnp.mean(widened * widened, axis=1, keepdims=True) + EPSILON)
    scaled = widened * inverse
    normed = (scaled * norm_gain).astype(jnp.bfloat16)
    logits = jnp.dot(normed, router_weight, preferred_element_type=jnp.float32)
    labels = jnp.arange(experts, dtype=jnp.int32)
    member = jnp.any(expert_ids[:, :, None] == labels, axis=1)
    lifted = jnp.where(member, jnp.exp(jnp.where(member, logits, 0.0)), 0.0)
    gates = lifted / jnp.sum(lifted, axis=1, keepdims=True)
    earlier = (
        jnp.arange(rows_here)[:, None] > jnp.arange(rows_here)[None, :]
    ).astype(jnp.bfloat16)
    rank = jnp.dot(earlier, member.astype(jnp.bfloat16), preferred_element_type=jnp.float32)
    rank = jnp.where(member, rank, -1.0).T

    def slots_of(first, count):
        block = jnp.repeat(rank, count, axis=0)
        slot = jnp.arange(experts * count, dtype=jnp.int32) % count + first
        return block == slot.astype(jnp.float32)[:, None]

    both = jnp.concatenate([normed, cotangent], axis=1)

    def dispatched(pick, slots):
        gate = jnp.sum(jnp.where(pick, jnp.repeat(gates.T, slots, axis=0), 0.0), axis=1)
        moved = jnp.dot(pick.astype(jnp.bfloat16), both, preferred_element_type=jnp.float32)
        is_upstream = jnp.arange(2 * width) >= width
        moved = moved * jnp.where(is_upstream[None, :], gate[:, None], 1.0)
        return moved.astype(jnp.bfloat16).reshape(experts, slots, 2 * width)

    picks = [slots_of(0, SLOTS), slots_of(SLOTS, EXTRA)]
    out_main = dispatched(picks[0], SLOTS)
    out_extra = dispatched(picks[1], EXTRA)
    picks = [pick.astype(jnp.bfloat16) for pick in picks]

    def pick_expert(w, which):
        return lax.dynamic_index_in_dim(w, which, 0, keepdims=False)

    weights = (gate_weight, up_weight, down_weight)
    (main, extra), theirs = exchange(
        [out_main, out_extra],
        [pick_expert(w, 1 - core) for w in weights],
        [],
        expert_of,
        linear,
        1,
    )
    arrived = jnp.concatenate(
        [main.reshape(DEVICES * SLOTS, 2 * width), extra.reshape(DEVICES * EXTRA, 2 * width)]
    )
    ours = [pick_expert(w, core) for w in weights]
    parts, back, score = expert_pass(
        arrived[:, :width], arrived[:, width:], *[(a, b) for a, b in zip(ours, theirs)]
    )
    back = back.astype(jnp.bfloat16)
    edge = DEVICES * SLOTS
    score_high = score.astype(jnp.bfloat16)
    score_low = (score - score_high.astype(jnp.float32)).astype(jnp.bfloat16)
    lane = jnp.arange(128)
    at = jnp.arange(score.shape[0])
    slot_lane = jnp.where(at < edge, at % SLOTS, SLOTS + (at - edge) % EXTRA)
    sender = jnp.where(at < edge, at // SLOTS, (at - edge) // EXTRA)
    spread_out = (slot_lane[:, None] == lane[None, :]).astype(jnp.bfloat16)
    group = (sender[None, :] == jnp.arange(DEVICES)[:, None]).astype(jnp.bfloat16)

    def lanes(part):
        return jnp.dot(group, part[:, None] * spread_out, preferred_element_type=jnp.float32)

    tail = jnp.stack([lanes(score_high), lanes(score_low)], axis=1).astype(jnp.bfloat16)
    (home_main, home_extra), grads = exchange(
        [
            back[:edge].reshape(DEVICES, SLOTS, width),
            jnp.concatenate([back[edge:].reshape(DEVICES, EXTRA, width), tail], axis=2),
        ],
        list(parts[1]),
        list(parts[0]),
        linear,
        half_and_expert,
        2,
    )
    home_main = home_main.reshape(2 * experts * SLOTS, width)
    tails = jnp.sum(home_extra[:, :, width:].astype(jnp.float32), axis=1)
    slot_score = tails[:experts] + tails[experts:]
    home_extra = home_extra[:, :, :width].reshape(2 * experts * EXTRA, width)
    grad_tok = jnp.dot(
        jnp.concatenate([picks[0], picks[0]]).T, home_main, preferred_element_type=jnp.float32
    ) + jnp.dot(
        jnp.concatenate([picks[1], picks[1]]).T, home_extra, preferred_element_type=jnp.float32
    )
    score_te = sum(
        jnp.where(rank == float(slot), slot_score[:, slot][:, None], 0.0)
        for slot in range(SLOTS + EXTRA)
    ).T
    grad_logits = (score_te - gates * jnp.sum(score_te, axis=1, keepdims=True)).astype(jnp.bfloat16)
    grad_normed = grad_tok + jnp.dot(
        grad_logits, router_weight.T, preferred_element_type=jnp.float32
    )
    router_part = jnp.dot(normed.T, grad_logits, preferred_element_type=jnp.float32)
    gain_part = jnp.sum(grad_normed * scaled, axis=0)
    sums = jnp.concatenate([router_part, gain_part[:, None]], axis=1)
    sums = sums.reshape(DEVICES, width // DEVICES, experts + 1)
    sums = lax.all_to_all(sums, ("dp", "ctx"), split_axis=0, concat_axis=0, tiled=True)
    sums = jnp.sum(sums, axis=0)
    grad_scaled = grad_normed * norm_gain
    correction = jnp.mean(grad_scaled * scaled, axis=1, keepdims=True)
    grad_input = (
        cotangent.astype(jnp.float32) + inverse * (grad_scaled - scaled * correction)
    ).astype(jnp.bfloat16)
    return (grad_input, *grads, sums[:, :experts], sums[:, experts])


def solution(mesh):
    return jax.shard_map(
        body,
        mesh=mesh,
        in_specs=(
            P(("dp", "ctx"), None),
            P(("dp", "ctx"), None),
            P(("dp", "ctx"), None),
            P(),
            P(),
            P("ctx", None, "dp"),
            P("ctx", None, "dp"),
            P("ctx", "dp", None),
        ),
        out_specs=(
            P(("dp", "ctx"), None),
            P("ctx", None, "dp"),
            P("ctx", None, "dp"),
            P("ctx", "dp", None),
            P(("dp", "ctx"), None),
            P(("dp", "ctx")),
        ),
        check_vma=False,
    )
```

```python
import functools

import jax
import jax.numpy as jnp
from jax import lax
from jax.experimental import pallas as pl
from jax.experimental.pallas import tpu as pltpu
from jax.sharding import PartitionSpec as P

EPSILON = 1e-05
SWISH_SCALE = 1.702
MESH = pl.DeviceIdType.MESH
SLOTS = 8
EXTRA = 2
ROW_BLOCK = 256
DEVICES = 128


def coordinates():
    dp, ctx = lax.axis_index("dp"), lax.axis_index("ctx")
    return (ctx // 4) % 4, ctx % 4, (dp // 2) * 2 + ctx // 16, dp % 2


def device_of(x, y, z, core):
    return (z // 2) * 2 + core, (z % 2) * 16 + x * 4 + y


def exchange_kernel(count, swaps, source_block, target_block, *refs):
    sends, refs = refs[:count], refs[count:]
    gives, refs = refs[:swaps], refs[swaps:]
    lands, refs = refs[:count], refs[count:]
    takes, refs = refs[:swaps], refs[swaps:]
    send_sem, recv_sem, local_sem, swap_send, swap_recv = refs
    x, y, z, core = coordinates()
    partner = device_of(x, y, z, 1 - core)
    swapped = [
        pltpu.make_async_remote_copy(
            src_ref=gives[i].at[1 - core],
            dst_ref=takes[i],
            send_sem=swap_send.at[i],
            recv_sem=swap_recv.at[i],
            device_id=partner,
            device_id_type=MESH,
        )
        for i in range(swaps)
    ]
    to_all(sends, lands, source_block, target_block, send_sem, recv_sem, local_sem, swapped)


def to_all(sends, lands, source_block, target_block, send_sem, recv_sem, local_sem, swapped, work=None):
    count = len(sends)
    x, y, z, core = coordinates()
    mine = device_of(x, y, z, core)

    sign = 1 - 2 * core

    def peer(k):
        return device_of(
            (x + sign * k + DEVICES) % 4,
            (y + sign * (3 * k + k // 4) + 4 * DEVICES) % 4,
            (z + sign * (2 * k + k // 4 + k // 16) + 4 * DEVICES) % 4,
            (core + k // 64 + k // 4) % 2,
        )

    barrier = pltpu.get_barrier_semaphore()

    def greet(k, carry):
        pl.semaphore_signal(barrier, inc=1, device_id=peer(k), device_id_type=MESH)
        return carry

    lax.fori_loop(1, DEVICES, greet, 0)
    pl.semaphore_wait(barrier, DEVICES - 1)

    def copy(i, k, slot):
        dp, ctx = peer(k)
        return pltpu.make_async_remote_copy(
            src_ref=sends[i].at[source_block(dp, ctx)],
            dst_ref=lands[i].at[slot],
            send_sem=send_sem.at[i, k],
            recv_sem=recv_sem.at[i, slot],
            device_id=(dp, ctx),
            device_id_type=MESH,
        )

    own_slot = target_block(*mine)
    kept = [
        pltpu.make_async_copy(
            sends[i].at[source_block(*mine)], lands[i].at[own_slot], local_sem.at[i]
        )
        for i in range(count)
    ]

    def start(k, carry):
        for i in range(count):
            copy(i, k, own_slot).start()
        return carry

    lax.fori_loop(1, DEVICES, start, 0)
    for item in swapped + kept:
        item.start()
    if work is not None:
        work()

    def finish(k, carry):
        slot = target_block(*peer(k))
        for i in range(count):
            copy(i, k, slot).wait()
        return carry

    lax.fori_loop(1, DEVICES, finish, 0)
    for item in swapped + kept:
        item.wait()


def semaphores(count):
    return [
        pltpu.SemaphoreType.DMA((count, DEVICES)),
        pltpu.SemaphoreType.DMA((count, DEVICES)),
        pltpu.SemaphoreType.DMA((count,)),
        pltpu.SemaphoreType.DMA((3,)),
        pltpu.SemaphoreType.DMA((3,)),
    ]


def exchange(sends, gives, source_block, target_block, collective_id):
    count, swaps = len(sends), len(gives)
    anywhere = pl.BlockSpec(memory_space=pl.ANY)
    out = pl.pallas_call(
        functools.partial(exchange_kernel, count, swaps, source_block, target_block),
        out_shape=[jax.ShapeDtypeStruct((DEVICES,) + a.shape[1:], a.dtype) for a in sends]
        + [jax.ShapeDtypeStruct(a.shape[1:], a.dtype) for a in gives],
        in_specs=[anywhere] * (count + swaps),
        out_specs=[anywhere] * (count + swaps),
        scratch_shapes=semaphores(count),
        compiler_params=pltpu.CompilerParams(
            collective_id=collective_id, has_side_effects=True
        ),
    )(*sends, *gives)
    return out[:count], out[count:]


def expert_of(dp, ctx):
    return 2 * ctx + dp % 2


def linear(dp, ctx):
    return dp * 32 + ctx


def half_and_expert(dp, ctx):
    return (dp // 2) * 64 + expert_of(dp, ctx)


def dot(a, b, contract):
    return lax.dot_general(a, b, (contract, ((), ())), preferred_element_type=jnp.float32)


def expert_kernel(
    main, extra, gate_own, up_own, down_own, gate_other, up_other, down_other,
    hidden_out, gate_out, up_out, back_out, score_out,
    rows, w_gate, w_up, w_down, sem,
):
    core = lax.axis_index("dp") % 2
    half = w_down.shape[0] // 2
    width = w_down.shape[1]
    top = main.shape[0]
    copies = [
        pltpu.make_async_copy(main, rows.at[pl.ds(0, top)], sem.at[0]),
        pltpu.make_async_copy(extra, rows.at[pl.ds(top, extra.shape[0])], sem.at[1]),
        pltpu.make_async_copy(gate_own.at[core], w_gate.at[:, pl.ds(0, half)], sem.at[2]),
        pltpu.make_async_copy(gate_other, w_gate.at[:, pl.ds(half, half)], sem.at[3]),
        pltpu.make_async_copy(up_own.at[core], w_up.at[:, pl.ds(0, half)], sem.at[4]),
        pltpu.make_async_copy(up_other, w_up.at[:, pl.ds(half, half)], sem.at[5]),
        pltpu.make_async_copy(down_own.at[core], w_down.at[pl.ds(0, half)], sem.at[6]),
        pltpu.make_async_copy(down_other, w_down.at[pl.ds(half, half)], sem.at[7]),
    ]
    for item in copies:
        item.start()
    for item in copies:
        item.wait()

    def step(i, carry):
        block = pl.ds(pl.multiple_of(i * ROW_BLOCK, ROW_BLOCK), ROW_BLOCK)
        normed = rows[block, :width]
        upstream = rows[block, width:]
        gate_pre = dot(normed, w_gate[...], ((1,), (0,)))
        up_pre = dot(normed, w_up[...], ((1,), (0,))) + 1.0
        grad_hidden = dot(upstream, w_down[...], ((1,), (1,)))
        squash = jax.nn.sigmoid(SWISH_SCALE * gate_pre)
        swish = gate_pre * squash
        hidden = (swish * up_pre).astype(jnp.bfloat16)
        slope = squash + SWISH_SCALE * swish * (1.0 - squash)
        pre_gate = (grad_hidden * up_pre * slope).astype(jnp.bfloat16)
        pre_up = (grad_hidden * swish).astype(jnp.bfloat16)
        hidden_out[block, :] = hidden
        gate_out[block, :] = pre_gate
        up_out[block, :] = pre_up
        score = jnp.sum(grad_hidden * hidden.astype(jnp.float32), axis=1, keepdims=True)
        score_out[block, :] = jnp.broadcast_to(score, (ROW_BLOCK, 128))
        back = dot(pre_gate, w_gate[...], ((1,), (1,))) + dot(pre_up, w_up[...], ((1,), (1,)))
        back_out[block, :] = back.astype(jnp.bfloat16)
        return carry

    lax.fori_loop(0, rows.shape[0] // ROW_BLOCK, step, 0)


def expert_pass(main, extra, weights, theirs):
    count = main.shape[0] + extra.shape[0]
    width, hidden = main.shape[1] // 2, 2 * theirs[2].shape[0]
    vmem = pl.BlockSpec(memory_space=pltpu.VMEM)
    anywhere = pl.BlockSpec(memory_space=pl.ANY)
    low = jnp.bfloat16
    return pl.pallas_call(
        expert_kernel,
        out_shape=[
            jax.ShapeDtypeStruct((count, hidden), low),
            jax.ShapeDtypeStruct((count, hidden), low),
            jax.ShapeDtypeStruct((count, hidden), low),
            jax.ShapeDtypeStruct((count, width), low),
            jax.ShapeDtypeStruct((count, 128), jnp.float32),
        ],
        in_specs=[anywhere] * 8,
        out_specs=[vmem] * 5,
        scratch_shapes=[
            pltpu.VMEM((count, 2 * width), low),
            pltpu.VMEM((width, hidden), low),
            pltpu.VMEM((width, hidden), low),
            pltpu.VMEM((hidden, width), low),
            pltpu.SemaphoreType.DMA((8,)),
        ],
        compiler_params=pltpu.CompilerParams(vmem_limit_bytes=60 * 2**20),
        cost_estimate=pl.CostEstimate(
            flops=10 * count * width * hidden, bytes_accessed=40 * 2**20, transcendentals=count * hidden
        ),
    )(main, extra, *weights, *theirs)


TILE = 256


def home_kernel(
    back_main, back_extra, main, extra, hidden, pre_gate, pre_up,
    home_main, home_extra, gate_grad, up_grad, down_grad,
    rows, hid, gat, upp, gate_buf, up_buf, down_buf, load_sem,
    send_sem, recv_sem, local_sem, swap_send, swap_recv,
):
    x, y, z, core = coordinates()
    partner = device_of(x, y, z, 1 - core)
    half = hid.shape[1] // 2
    width = down_buf.shape[1]
    top = main.shape[0]
    bufs, outs = (gate_buf, up_buf, down_buf), (gate_grad, up_grad, down_grad)

    def part(buf, i):
        at = pl.ds(i * half, half)
        return buf.at[at] if buf is down_buf else buf.at[:, at]

    def work():
        loads = [
            pltpu.make_async_copy(main, rows.at[pl.ds(0, top)], load_sem.at[0]),
            pltpu.make_async_copy(extra, rows.at[pl.ds(top, extra.shape[0])], load_sem.at[1]),
            pltpu.make_async_copy(hidden, hid, load_sem.at[2]),
            pltpu.make_async_copy(pre_gate, gat, load_sem.at[3]),
            pltpu.make_async_copy(pre_up, upp, load_sem.at[4]),
        ]
        for item in loads:
            item.start()
        for item in loads:
            item.wait()

        def columns(i, carry):
            at = pl.ds(pl.multiple_of(i * TILE, TILE), TILE)
            tile = rows[:, at]
            gate_buf[at, :] = dot(tile, gat[...], ((0,), (0,))).astype(jnp.bfloat16)
            up_buf[at, :] = dot(tile, upp[...], ((0,), (0,))).astype(jnp.bfloat16)
            return carry

        lax.fori_loop(0, width // TILE, columns, 0)

        def units(i, carry):
            at = pl.ds(pl.multiple_of(i * TILE, TILE), TILE)
            down_buf[at, :] = dot(hid[:, at], rows[:, width:], ((0,), (0,))).astype(jnp.bfloat16)
            return carry

        lax.fori_loop(0, down_buf.shape[0] // TILE, units, 0)
        moves = []
        for i, (buf, out) in enumerate(zip(bufs, outs)):
            moves.append(pltpu.make_async_remote_copy(
                src_ref=part(buf, 1),
                dst_ref=out.at[core],
                send_sem=swap_send.at[i],
                recv_sem=swap_recv.at[i],
                device_id=partner,
                device_id_type=MESH,
            ))
            moves.append(pltpu.make_async_copy(part(buf, 0), out.at[core], load_sem.at[i]))
        for item in moves:
            item.start()
        for item in moves:
            item.wait()

    to_all(
        (back_main, back_extra), (home_main, home_extra), linear, half_and_expert,
        send_sem, recv_sem, local_sem, [], work,
    )


def send_home(back_main, back_extra, main, extra, hidden, pre_gate, pre_up):
    count, units = hidden.shape
    width = main.shape[1] // 2
    half = units // 2
    low = jnp.bfloat16
    anywhere = pl.BlockSpec(memory_space=pl.ANY)
    return pl.pallas_call(
        home_kernel,
        out_shape=[
            jax.ShapeDtypeStruct(back_main.shape, low),
            jax.ShapeDtypeStruct(back_extra.shape, low),
            jax.ShapeDtypeStruct((2, width, half), low),
            jax.ShapeDtypeStruct((2, width, half), low),
            jax.ShapeDtypeStruct((2, half, width), low),
        ],
        in_specs=[anywhere] * 7,
        out_specs=[anywhere] * 5,
        scratch_shapes=[
            pltpu.VMEM((count, 2 * width), low),
            pltpu.VMEM((count, units), low),
            pltpu.VMEM((count, units), low),
            pltpu.VMEM((count, units), low),
            pltpu.VMEM((width, units), low),
            pltpu.VMEM((width, units), low),
            pltpu.VMEM((units, width), low),
            pltpu.SemaphoreType.DMA((5,)),
            *semaphores(2),
        ],
        compiler_params=pltpu.CompilerParams(
            collective_id=2, has_side_effects=True, vmem_limit_bytes=60 * 2**20
        ),
    )(back_main, back_extra, main, extra, hidden, pre_gate, pre_up)


def body(
    tokens, cotangent, expert_ids, norm_gain, router_weight, gate_weight, up_weight, down_weight
):
    experts = router_weight.shape[1]
    rows_here, width = tokens.shape
    widened = tokens.astype(jnp.float32)
    inverse = lax.rsqrt(jnp.mean(widened * widened, axis=1, keepdims=True) + EPSILON)
    scaled = widened * inverse
    normed = (scaled * norm_gain).astype(jnp.bfloat16)
    logits = jnp.dot(normed, router_weight, preferred_element_type=jnp.float32)
    labels = jnp.arange(experts, dtype=jnp.int32)
    member = jnp.any(expert_ids[:, :, None] == labels, axis=1)
    lifted = jnp.where(member, jnp.exp(jnp.where(member, logits, 0.0)), 0.0)
    gates = lifted / jnp.sum(lifted, axis=1, keepdims=True)
    earlier = (
        jnp.arange(rows_here)[:, None] > jnp.arange(rows_here)[None, :]
    ).astype(jnp.bfloat16)
    rank = jnp.dot(earlier, member.astype(jnp.bfloat16), preferred_element_type=jnp.float32)
    rank = jnp.where(member, rank, -1.0).T

    def slots_of(first, count):
        block = jnp.repeat(rank, count, axis=0)
        slot = jnp.arange(experts * count, dtype=jnp.int32) % count + first
        return block == slot.astype(jnp.float32)[:, None]

    both = jnp.concatenate([normed, cotangent], axis=1)

    def dispatched(pick, slots):
        gate = jnp.sum(jnp.where(pick, jnp.repeat(gates.T, slots, axis=0), 0.0), axis=1)
        moved = jnp.dot(pick.astype(jnp.bfloat16), both, preferred_element_type=jnp.float32)
        is_upstream = jnp.arange(2 * width) >= width
        moved = moved * jnp.where(is_upstream[None, :], gate[:, None], 1.0)
        return moved.astype(jnp.bfloat16).reshape(experts, slots, 2 * width)

    picks = [slots_of(0, SLOTS), slots_of(SLOTS, EXTRA)]
    out_main = dispatched(picks[0], SLOTS)
    out_extra = dispatched(picks[1], EXTRA)
    picks = [pick.astype(jnp.bfloat16) for pick in picks]

    weights = (gate_weight, up_weight, down_weight)
    (main, extra), theirs = exchange([out_main, out_extra], weights, expert_of, linear, 1)
    main = main.reshape(DEVICES * SLOTS, 2 * width)
    extra = extra.reshape(DEVICES * EXTRA, 2 * width)
    hidden, pre_gate, pre_up, back, score = expert_pass(main, extra, weights, theirs)
    edge = DEVICES * SLOTS
    score = score[:, 0]
    score_high = score.astype(jnp.bfloat16)
    score_low = (score - score_high.astype(jnp.float32)).astype(jnp.bfloat16)
    lane = jnp.arange(128)
    at = jnp.arange(score.shape[0])
    slot_lane = jnp.where(at < edge, at % SLOTS, SLOTS + (at - edge) % EXTRA)
    sender = jnp.where(at < edge, at // SLOTS, (at - edge) // EXTRA)
    spread_out = (slot_lane[:, None] == lane[None, :]).astype(jnp.bfloat16)
    group = (sender[None, :] == jnp.arange(DEVICES)[:, None]).astype(jnp.bfloat16)

    def lanes(part):
        return jnp.dot(group, part[:, None] * spread_out, preferred_element_type=jnp.float32)

    tail = jnp.stack([lanes(score_high), lanes(score_low)], axis=1).astype(jnp.bfloat16)
    home_main, home_extra, *grads = send_home(
        back[:edge].reshape(DEVICES, SLOTS, width),
        jnp.concatenate([back[edge:].reshape(DEVICES, EXTRA, width), tail], axis=2),
        main,
        extra,
        hidden,
        pre_gate,
        pre_up,
    )
    home_main = home_main.reshape(2 * experts * SLOTS, width)
    tails = jnp.sum(home_extra[:, :, width:].astype(jnp.float32), axis=1)
    slot_score = tails[:experts] + tails[experts:]
    home_extra = home_extra[:, :, :width].reshape(2 * experts * EXTRA, width)
    grad_tok = jnp.dot(
        jnp.concatenate([picks[0], picks[0]]).T, home_main, preferred_element_type=jnp.float32
    ) + jnp.dot(
        jnp.concatenate([picks[1], picks[1]]).T, home_extra, preferred_element_type=jnp.float32
    )
    score_te = sum(
        jnp.where(rank == float(slot), slot_score[:, slot][:, None], 0.0)
        for slot in range(SLOTS + EXTRA)
    ).T
    grad_logits = (score_te - gates * jnp.sum(score_te, axis=1, keepdims=True)).astype(jnp.bfloat16)
    grad_normed = grad_tok + jnp.dot(
        grad_logits, router_weight.T, preferred_element_type=jnp.float32
    )
    router_part = jnp.dot(normed.T, grad_logits, preferred_element_type=jnp.float32)
    gain_part = jnp.sum(grad_normed * scaled, axis=0)
    sums = jnp.concatenate([router_part, gain_part[:, None]], axis=1)
    sums = sums.reshape(DEVICES, width // DEVICES, experts + 1)
    sums = lax.all_to_all(sums, ("dp", "ctx"), split_axis=0, concat_axis=0, tiled=True)
    sums = jnp.sum(sums, axis=0)
    grad_scaled = grad_normed * norm_gain
    correction = jnp.mean(grad_scaled * scaled, axis=1, keepdims=True)
    grad_input = (
        cotangent.astype(jnp.float32) + inverse * (grad_scaled - scaled * correction)
    ).astype(jnp.bfloat16)
    return (grad_input, *grads, sums[:, :experts], sums[:, experts])


def solution(mesh):
    return jax.shard_map(
        body,
        mesh=mesh,
        in_specs=(
            P(("dp", "ctx"), None),
            P(("dp", "ctx"), None),
            P(("dp", "ctx"), None),
            P(),
            P(),
            P("ctx", None, "dp"),
            P("ctx", None, "dp"),
            P("ctx", "dp", None),
        ),
        out_specs=(
            P(("dp", "ctx"), None),
            P("ctx", None, "dp"),
            P("ctx", None, "dp"),
            P("ctx", "dp", None),
            P(("dp", "ctx"), None),
            P(("dp", "ctx")),
        ),
        check_vma=False,
    )
```

```python
import functools

import jax
import jax.numpy as jnp
from jax import lax
from jax.experimental import pallas as pl
from jax.experimental.pallas import tpu as pltpu
from jax.sharding import PartitionSpec as P

EPSILON = 1e-05
SWISH_SCALE = 1.702
MESH = pl.DeviceIdType.MESH
SLOTS = 8
EXTRA = 2
ROW_BLOCK = 256
DEVICES = 128


def coordinates():
    dp, ctx = lax.axis_index("dp"), lax.axis_index("ctx")
    return (ctx // 4) % 4, ctx % 4, (dp // 2) * 2 + ctx // 16, dp % 2


def device_of(x, y, z, core):
    return (z // 2) * 2 + core, (z % 2) * 16 + x * 4 + y


def expert_of(dp, ctx):
    return 2 * ctx + dp % 2


def half_and_expert(dp, ctx):
    return (dp // 2) * 64 + expert_of(dp, ctx)


def dot(a, b, contract):
    return lax.dot_general(a, b, (contract, ((), ())), preferred_element_type=jnp.float32)


def moe_kernel(
    out_main, out_extra, gate_weight, up_weight, down_weight,
    home_main, home_extra, gate_grad, up_grad, down_grad,
    rows, back, w_gate, w_up, w_down, hid, gat, upp, gate_buf, up_buf, down_buf,
    go_send, go_recv, home_send, home_recv, local_sem, load_sem,
    weight_send, weight_recv, grad_send, grad_recv,
):
    x, y, z, core = coordinates()
    mine = device_of(x, y, z, core)
    partner = device_of(x, y, z, 1 - core)
    edge = DEVICES * SLOTS
    half = down_weight.shape[1]
    width = down_weight.shape[2]

    def turn(k, sign, flip):
        return device_of(
            (x + sign * k + DEVICES) % 4,
            (y + sign * (3 * k + k // 4) + 4 * DEVICES) % 4,
            (z + sign * (2 * k + k // 4 + k // 16) + 4 * DEVICES) % 4,
            flip,
        )

    def target(k):
        return turn(k, 1 - 2 * core, (core + k // 64 + k // 4) % 2)

    def source(k):
        other = (core + k // 64 + k // 4) % 2
        return turn(k, 2 * other - 1, other)

    def main_slot(ref, i):
        return ref.at[pl.ds(pl.multiple_of(i * SLOTS, SLOTS), SLOTS)]

    def extra_slot(ref, i, first=0):
        return ref.at[pl.ds(pl.multiple_of(first + i * EXTRA, EXTRA), EXTRA)]

    barrier = pltpu.get_barrier_semaphore()

    def greet(k, carry):
        pl.semaphore_signal(barrier, inc=1, device_id=target(k), device_id_type=MESH)
        return carry

    lax.fori_loop(1, DEVICES, greet, 0)
    pl.semaphore_wait(barrier, DEVICES - 1)

    def remote(src, dst, send, recv, device):
        return pltpu.make_async_remote_copy(
            src_ref=src, dst_ref=dst, send_sem=send, recv_sem=recv,
            device_id=device, device_id_type=MESH,
        )

    def go_main(k):
        to = target(k)
        return remote(
            main_slot(out_main, expert_of(*to)), main_slot(rows, k),
            go_send.at[0, k], go_recv.at[0, k], to,
        )

    def go_extra(k):
        to = target(k)
        return remote(
            extra_slot(out_extra, expert_of(*to)), extra_slot(rows, k, edge),
            go_send.at[1, k], go_recv.at[1, k], to,
        )

    def home_copy(k, to, index, kind):
        if kind == 0:
            src, dst = main_slot(back, k), main_slot(home_main, index)
        else:
            src, dst = extra_slot(back, k, edge), extra_slot(home_extra, index)
        return remote(src, dst, home_send.at[kind, k], home_recv.at[kind, index], to)

    own_index = half_and_expert(*mine)

    def return_main(k, carry):
        home_copy(k, source(k), own_index, 0).start()
        return carry

    def return_extra(k, carry):
        home_copy(k, source(k), own_index, 1).start()
        return carry

    places = (w_gate, w_up, w_down)

    def part(buf, i):
        at = pl.ds(i * half, half)
        return buf.at[at] if buf.shape[0] == 2 * half else buf.at[:, at]

    loads = []
    for i, (weight, place) in enumerate(zip((gate_weight, up_weight, down_weight), places)):
        loads.append(remote(
            weight.at[1 - core], part(place, 1), weight_send.at[i], weight_recv.at[i], partner
        ))
        loads.append(pltpu.make_async_copy(weight.at[core], part(place, 0), load_sem.at[i]))
    own = expert_of(*mine)
    loads.append(pltpu.make_async_copy(main_slot(out_main, own), main_slot(rows, 0), local_sem.at[0]))
    loads.append(
        pltpu.make_async_copy(extra_slot(out_extra, own), extra_slot(rows, 0, edge), local_sem.at[1])
    )

    def go(k, carry):
        go_main(k).start()
        go_extra(k).start()
        return carry

    for item in loads:
        item.start()
    lax.fori_loop(1, DEVICES, go, 0)
    for item in loads:
        item.wait()

    def main_came(k, carry):
        go_main(k).wait_recv()
        return carry

    def extra_came(k, carry):
        go_extra(k).wait_recv()
        return carry

    senders = ROW_BLOCK // SLOTS
    blocks = edge // ROW_BLOCK

    def step(i, carry):
        first = i * senders
        lax.fori_loop(jnp.maximum(first, 1), jnp.minimum(first + senders, DEVICES), main_came, 0)
        lax.fori_loop(DEVICES - (i // blocks) * (DEVICES - 1), DEVICES, extra_came, 0)
        block = pl.ds(pl.multiple_of(i * ROW_BLOCK, ROW_BLOCK), ROW_BLOCK)
        normed = rows[block, :width]
        upstream = rows[block, width:]
        gate_pre = dot(normed, w_gate[...], ((1,), (0,)))
        up_pre = dot(normed, w_up[...], ((1,), (0,))) + 1.0
        grad_hidden = dot(upstream, w_down[...], ((1,), (1,)))
        squash = jax.nn.sigmoid(SWISH_SCALE * gate_pre)
        swish = gate_pre * squash
        hidden = (swish * up_pre).astype(jnp.bfloat16)
        slope = squash + SWISH_SCALE * swish * (1.0 - squash)
        pre_gate = (grad_hidden * up_pre * slope).astype(jnp.bfloat16)
        pre_up = (grad_hidden * swish).astype(jnp.bfloat16)
        hid[block, :] = hidden
        gat[block, :] = pre_gate
        upp[block, :] = pre_up
        score = jnp.sum(grad_hidden * hidden.astype(jnp.float32), axis=1, keepdims=True)
        high = score.astype(jnp.bfloat16).astype(jnp.float32)
        lane = lax.broadcasted_iota(jnp.int32, (ROW_BLOCK, 128), 1)
        tail = jnp.where(lane == 0, high, jnp.where(lane == 1, score - high, 0.0))
        total = dot(pre_gate, w_gate[...], ((1,), (1,))) + dot(pre_up, w_up[...], ((1,), (1,)))
        back[block, :width] = total.astype(jnp.bfloat16)
        back[block, width:] = tail.astype(jnp.bfloat16)
        lax.fori_loop(jnp.maximum(first - senders, 1), first, return_main, 0)
        return carry

    lax.fori_loop(0, blocks + 1, step, 0)

    def columns(i, carry):
        at = pl.ds(pl.multiple_of(i * TILE, TILE), TILE)
        tile = rows[:, at]
        gate_buf[at, :] = dot(tile, gat[...], ((0,), (0,))).astype(jnp.bfloat16)
        up_buf[at, :] = dot(tile, upp[...], ((0,), (0,))).astype(jnp.bfloat16)
        return carry

    def units(i, carry):
        at = pl.ds(pl.multiple_of(i * TILE, TILE), TILE)
        down_buf[at, :] = dot(hid[:, at], rows[:, width:], ((0,), (0,))).astype(jnp.bfloat16)
        return carry

    lax.fori_loop(0, 1, units, 0)
    lax.fori_loop(1, DEVICES, return_extra, 0)
    kept = [
        pltpu.make_async_copy(main_slot(back, 0), main_slot(home_main, own_index), local_sem.at[0]),
        pltpu.make_async_copy(
            extra_slot(back, 0, edge), extra_slot(home_extra, own_index), local_sem.at[1]
        ),
    ]
    for item in kept:
        item.start()
    lax.fori_loop(1, 2 * half // TILE, units, 0)
    lax.fori_loop(0, width // TILE, columns, 0)
    grads = zip((down_buf, gate_buf, up_buf), (down_grad, gate_grad, up_grad))
    for i, (buf, out) in enumerate(grads):
        kept.append(remote(part(buf, 1), out.at[core], grad_send.at[i], grad_recv.at[i], partner))
        kept.append(pltpu.make_async_copy(part(buf, 0), out.at[core], load_sem.at[i]))
    for item in kept[2:]:
        item.start()

    def finish(k, carry):
        go_main(k).wait_send()
        go_extra(k).wait_send()
        index = half_and_expert(*target(k))
        for kind in range(2):
            home_copy(k, source(k), own_index, kind).wait_send()
            home_copy(k, source(k), index, kind).wait_recv()
        return carry

    lax.fori_loop(1, DEVICES, finish, 0)
    for item in kept:
        item.wait()


TILE = 256


def moe(out_main, out_extra, weights):
    half, width = weights[2].shape[1:]
    units = 2 * half
    count = DEVICES * (SLOTS + EXTRA)
    low = jnp.bfloat16
    anywhere = pl.BlockSpec(memory_space=pl.ANY)
    pair = pltpu.SemaphoreType.DMA((2, DEVICES))
    three = pltpu.SemaphoreType.DMA((3,))
    return pl.pallas_call(
        moe_kernel,
        out_shape=[
            jax.ShapeDtypeStruct((DEVICES * SLOTS, width + 128), low),
            jax.ShapeDtypeStruct((DEVICES * EXTRA, width + 128), low),
            jax.ShapeDtypeStruct((2, width, half), low),
            jax.ShapeDtypeStruct((2, width, half), low),
            jax.ShapeDtypeStruct((2, half, width), low),
        ],
        in_specs=[anywhere] * 5,
        out_specs=[anywhere] * 5,
        scratch_shapes=[
            pltpu.VMEM((count, 2 * width), low),
            pltpu.VMEM((count, width + 128), low),
            pltpu.VMEM((width, units), low),
            pltpu.VMEM((width, units), low),
            pltpu.VMEM((units, width), low),
            pltpu.VMEM((count, units), low),
            pltpu.VMEM((count, units), low),
            pltpu.VMEM((count, units), low),
            pltpu.VMEM((width, units), low),
            pltpu.VMEM((width, units), low),
            pltpu.VMEM((units, width), low),
            pair, pair, pair, pair,
            pltpu.SemaphoreType.DMA((2,)),
            three, three, three, three, three,
        ],
        compiler_params=pltpu.CompilerParams(
            collective_id=1, has_side_effects=True, vmem_limit_bytes=60 * 2**20
        ),
    )(out_main, out_extra, *weights)


def body(
    tokens, cotangent, expert_ids, norm_gain, router_weight, gate_weight, up_weight, down_weight
):
    experts = router_weight.shape[1]
    rows_here, width = tokens.shape
    widened = tokens.astype(jnp.float32)
    inverse = lax.rsqrt(jnp.mean(widened * widened, axis=1, keepdims=True) + EPSILON)
    scaled = widened * inverse
    normed = (scaled * norm_gain).astype(jnp.bfloat16)
    logits = jnp.dot(normed, router_weight, preferred_element_type=jnp.float32)
    labels = jnp.arange(experts, dtype=jnp.int32)
    member = jnp.any(expert_ids[:, :, None] == labels, axis=1)
    lifted = jnp.where(member, jnp.exp(jnp.where(member, logits, 0.0)), 0.0)
    gates = lifted / jnp.sum(lifted, axis=1, keepdims=True)
    earlier = (
        jnp.arange(rows_here)[:, None] > jnp.arange(rows_here)[None, :]
    ).astype(jnp.bfloat16)
    rank = jnp.dot(earlier, member.astype(jnp.bfloat16), preferred_element_type=jnp.float32)
    rank = jnp.where(member, rank, -1.0).T

    def slots_of(first, count):
        block = jnp.repeat(rank, count, axis=0)
        slot = jnp.arange(experts * count, dtype=jnp.int32) % count + first
        return block == slot.astype(jnp.float32)[:, None]

    both = jnp.concatenate([normed, cotangent], axis=1)

    def dispatched(pick, slots):
        gate = jnp.sum(jnp.where(pick, jnp.repeat(gates.T, slots, axis=0), 0.0), axis=1)
        moved = jnp.dot(pick.astype(jnp.bfloat16), both, preferred_element_type=jnp.float32)
        is_upstream = jnp.arange(2 * width) >= width
        moved = moved * jnp.where(is_upstream[None, :], gate[:, None], 1.0)
        return moved.astype(jnp.bfloat16)

    picks = [slots_of(0, SLOTS), slots_of(SLOTS, EXTRA)]
    out_main = dispatched(picks[0], SLOTS)
    out_extra = dispatched(picks[1], EXTRA)
    picks = [pick.astype(jnp.bfloat16) for pick in picks]

    home_main, home_extra, *grads = moe(
        out_main, out_extra, (gate_weight, up_weight, down_weight)
    )

    def gathered(pick, home):
        return jnp.dot(
            jnp.concatenate([pick, pick]).T, home, preferred_element_type=jnp.float32
        )

    def scores(pick, home, slots):
        tail = jnp.sum(home[:, width:].astype(jnp.float32), axis=1, keepdims=True)
        tail = tail[: experts * slots] + tail[experts * slots :]
        return jnp.sum((pick * tail).reshape(experts, slots, rows_here), axis=1)

    total = gathered(picks[0], home_main) + gathered(picks[1], home_extra)
    grad_tok = total[:, :width]
    score_te = (scores(picks[0], home_main, SLOTS) + scores(picks[1], home_extra, EXTRA)).T
    grad_logits = (score_te - gates * jnp.sum(score_te, axis=1, keepdims=True)).astype(jnp.bfloat16)
    grad_normed = grad_tok + jnp.dot(
        grad_logits, router_weight.T, preferred_element_type=jnp.float32
    )
    router_part = jnp.dot(normed.T, grad_logits, preferred_element_type=jnp.float32)
    gain_part = jnp.sum(grad_normed * scaled, axis=0)
    sums = jnp.concatenate([router_part, gain_part[:, None]], axis=1)
    sums = sums.reshape(DEVICES, width // DEVICES, experts + 1)
    sums = lax.all_to_all(sums, ("dp", "ctx"), split_axis=0, concat_axis=0, tiled=True)
    sums = jnp.sum(sums, axis=0)
    grad_scaled = grad_normed * norm_gain
    correction = jnp.mean(grad_scaled * scaled, axis=1, keepdims=True)
    grad_input = (
        cotangent.astype(jnp.float32) + inverse * (grad_scaled - scaled * correction)
    ).astype(jnp.bfloat16)
    return (grad_input, *grads, sums[:, :experts], sums[:, experts])


def solution(mesh):
    return jax.shard_map(
        body,
        mesh=mesh,
        in_specs=(
            P(("dp", "ctx"), None),
            P(("dp", "ctx"), None),
            P(("dp", "ctx"), None),
            P(),
            P(),
            P("ctx", None, "dp"),
            P("ctx", None, "dp"),
            P("ctx", "dp", None),
        ),
        out_specs=(
            P(("dp", "ctx"), None),
            P("ctx", None, "dp"),
            P("ctx", None, "dp"),
            P("ctx", "dp", None),
            P(("dp", "ctx"), None),
            P(("dp", "ctx")),
        ),
        check_vma=False,
    )
```

```python
import functools

import jax
import jax.numpy as jnp
from jax import lax
from jax.experimental import pallas as pl
from jax.experimental.pallas import tpu as pltpu
from jax.sharding import PartitionSpec as P

EPSILON = 1e-05
SWISH_SCALE = 1.702
MESH = pl.DeviceIdType.MESH
SLOTS = 8
EXTRA = 2
ROW_BLOCK = 256
DEVICES = 128


def coordinates():
    dp, ctx = lax.axis_index("dp"), lax.axis_index("ctx")
    return (ctx // 4) % 4, ctx % 4, (dp // 2) * 2 + ctx // 16, dp % 2


def device_of(x, y, z, core):
    return (z // 2) * 2 + core, (z % 2) * 16 + x * 4 + y


def expert_of(dp, ctx):
    return 2 * ctx + dp % 2


def half_and_expert(dp, ctx):
    return (dp // 2) * 64 + expert_of(dp, ctx)


def dot(a, b, contract):
    return lax.dot_general(a, b, (contract, ((), ())), preferred_element_type=jnp.float32)


def moe_kernel(
    out_main, out_extra, gate_weight, up_weight, down_weight,
    pick_main, pick_extra, gates, tokens, cotangent, norm_gain, router_weight,
    grad_tokens, gate_grad, up_grad, down_grad, sums, bounce,
    home_main, home_extra, part_sums, all_sums, rows, back, w_gate, w_up, w_down, hid, gat, upp, gate_buf, up_buf, down_buf,
    go_send, go_recv, home_send, home_recv, local_sem, load_sem,
    weight_send, weight_recv, grad_send, grad_recv, sum_send, sum_recv,
):
    x, y, z, core = coordinates()
    mine = device_of(x, y, z, core)
    partner = device_of(x, y, z, 1 - core)
    edge = DEVICES * SLOTS
    half = down_weight.shape[1]
    width = down_weight.shape[2]

    def turn(k, sign, flip):
        return device_of(
            (x + sign * k + DEVICES) % 4,
            (y + sign * (3 * k + k // 4) + 4 * DEVICES) % 4,
            (z + sign * (2 * k + k // 4 + k // 16) + 4 * DEVICES) % 4,
            flip,
        )

    def target(k):
        return turn(k, 1 - 2 * core, (core + k // 64 + k // 4) % 2)

    def source(k):
        other = (core + k // 64 + k // 4) % 2
        return turn(k, 2 * other - 1, other)

    def main_slot(ref, i):
        return ref.at[pl.ds(pl.multiple_of(i * SLOTS, SLOTS), SLOTS)]

    def extra_slot(ref, i, first=0):
        return ref.at[pl.ds(pl.multiple_of(first + i * EXTRA, EXTRA), EXTRA)]

    barrier = pltpu.get_barrier_semaphore()

    def greet(k, carry):
        pl.semaphore_signal(barrier, inc=1, device_id=target(k), device_id_type=MESH)
        return carry

    lax.fori_loop(1, DEVICES, greet, 0)
    pl.semaphore_wait(barrier, DEVICES - 1)

    def remote(src, dst, send, recv, device):
        return pltpu.make_async_remote_copy(
            src_ref=src, dst_ref=dst, send_sem=send, recv_sem=recv,
            device_id=device, device_id_type=MESH,
        )

    def go_main(k):
        to = target(k)
        return remote(
            main_slot(out_main, expert_of(*to)), main_slot(rows, k),
            go_send.at[0, k], go_recv.at[0, k], to,
        )

    def go_extra(k):
        to = target(k)
        return remote(
            extra_slot(out_extra, expert_of(*to)), extra_slot(rows, k, edge),
            go_send.at[1, k], go_recv.at[1, k], to,
        )

    def home_copy(k, to, index, kind):
        if kind == 0:
            src, dst = main_slot(back, k), main_slot(home_main, index)
        else:
            src, dst = extra_slot(back, k, edge), extra_slot(home_extra, index)
        return remote(src, dst, home_send.at[kind, k], home_recv.at[kind, index], to)

    own_index = half_and_expert(*mine)

    def return_main(k, carry):
        home_copy(k, source(k), own_index, 0).start()
        return carry

    def return_extra(k, carry):
        home_copy(k, source(k), own_index, 1).start()
        return carry

    places = (w_gate, w_up, w_down)

    def part(buf, i):
        at = pl.ds(i * half, half)
        return buf.at[at] if buf.shape[0] == 2 * half else buf.at[:, at]

    loads = []
    for i, (weight, place) in enumerate(zip((gate_weight, up_weight, down_weight), places)):
        loads.append(remote(
            weight.at[1 - core], part(place, 1), weight_send.at[i], weight_recv.at[i], partner
        ))
        loads.append(pltpu.make_async_copy(weight.at[core], part(place, 0), load_sem.at[i]))
    own = expert_of(*mine)
    loads.append(pltpu.make_async_copy(main_slot(out_main, own), main_slot(rows, 0), local_sem.at[0]))
    loads.append(
        pltpu.make_async_copy(extra_slot(out_extra, own), extra_slot(rows, 0, edge), local_sem.at[1])
    )

    def go(k, carry):
        go_main(k).start()
        go_extra(k).start()
        return carry

    for item in loads:
        item.start()
    lax.fori_loop(1, DEVICES, go, 0)
    for item in loads:
        item.wait()

    def main_came(k, carry):
        go_main(k).wait_recv()
        return carry

    def extra_came(k, carry):
        go_extra(k).wait_recv()
        return carry

    senders = ROW_BLOCK // SLOTS
    blocks = edge // ROW_BLOCK

    def step(i, carry):
        first = i * senders
        lax.fori_loop(jnp.maximum(first, 1), jnp.minimum(first + senders, DEVICES), main_came, 0)
        lax.fori_loop(DEVICES - (i // blocks) * (DEVICES - 1), DEVICES, extra_came, 0)
        block = pl.ds(pl.multiple_of(i * ROW_BLOCK, ROW_BLOCK), ROW_BLOCK)
        normed = rows[block, :width]
        upstream = rows[block, width:]
        gate_pre = dot(normed, w_gate[...], ((1,), (0,)))
        up_pre = dot(normed, w_up[...], ((1,), (0,))) + 1.0
        grad_hidden = dot(upstream, w_down[...], ((1,), (1,)))
        squash = jax.nn.sigmoid(SWISH_SCALE * gate_pre)
        swish = gate_pre * squash
        hidden = (swish * up_pre).astype(jnp.bfloat16)
        slope = squash + SWISH_SCALE * swish * (1.0 - squash)
        pre_gate = (grad_hidden * up_pre * slope).astype(jnp.bfloat16)
        pre_up = (grad_hidden * swish).astype(jnp.bfloat16)
        hid[block, :] = hidden
        gat[block, :] = pre_gate
        upp[block, :] = pre_up
        score = jnp.sum(grad_hidden * hidden.astype(jnp.float32), axis=1, keepdims=True)
        high = score.astype(jnp.bfloat16).astype(jnp.float32)
        lane = lax.broadcasted_iota(jnp.int32, (ROW_BLOCK, 128), 1)
        tail = jnp.where(lane == 0, high, jnp.where(lane == 1, score - high, 0.0))
        total = dot(pre_gate, w_gate[...], ((1,), (1,))) + dot(pre_up, w_up[...], ((1,), (1,)))
        back[block, :width] = total.astype(jnp.bfloat16)
        back[block, width:] = tail.astype(jnp.bfloat16)
        lax.fori_loop(jnp.maximum(first - senders, 1), first, return_main, 0)
        return carry

    lax.fori_loop(0, blocks + 1, step, 0)

    def columns(i, carry):
        at = pl.ds(pl.multiple_of(i * TILE, TILE), TILE)
        tile = rows[:, at]
        gate_buf[at, :] = dot(tile, gat[...], ((0,), (0,))).astype(jnp.bfloat16)
        up_buf[at, :] = dot(tile, upp[...], ((0,), (0,))).astype(jnp.bfloat16)
        return carry

    def units(i, carry):
        at = pl.ds(pl.multiple_of(i * TILE, TILE), TILE)
        down_buf[at, :] = dot(hid[:, at], rows[:, width:], ((0,), (0,))).astype(jnp.bfloat16)
        return carry

    lax.fori_loop(0, 1, units, 0)
    lax.fori_loop(1, DEVICES, return_extra, 0)
    away = [
        pltpu.make_async_copy(main_slot(back, 0), main_slot(bounce, 0), local_sem.at[0]),
        pltpu.make_async_copy(extra_slot(back, 0, edge), extra_slot(bounce, 0, SLOTS), local_sem.at[1]),
    ]
    kept = [
        pltpu.make_async_copy(main_slot(bounce, 0), main_slot(home_main, own_index), local_sem.at[0]),
        pltpu.make_async_copy(
            extra_slot(bounce, 0, SLOTS), extra_slot(home_extra, own_index), local_sem.at[1]
        ),
    ]
    for item in away:
        item.start()
    lax.fori_loop(1, 2 * half // TILE, units, 0)
    for item in away:
        item.wait()
    for item in kept:
        item.start()
    lax.fori_loop(0, width // TILE, columns, 0)
    grads = zip((down_buf, gate_buf, up_buf), (down_grad, gate_grad, up_grad))
    moves = []
    for i, (buf, out) in enumerate(grads):
        moves.append(remote(part(buf, 1), out.at[core], grad_send.at[i], grad_recv.at[i], partner))
        moves.append(pltpu.make_async_copy(part(buf, 0), out.at[core], load_sem.at[i]))
    for item in moves:
        item.start()

    def home_came(k, carry):
        index = half_and_expert(*target(k))
        for kind in range(2):
            home_copy(k, source(k), index, kind).wait_recv()
        return carry

    lax.fori_loop(1, DEVICES, home_came, 0)
    for item in kept:
        item.wait()

    low, high = jnp.bfloat16, jnp.float32
    experts = router_weight.shape[1]
    total, score = None, None
    for pick, home, slots in ((pick_main, home_main, SLOTS), (pick_extra, home_extra, EXTRA)):
        count = experts * slots
        one_hot = pick[...]
        tail = home[:, width:].astype(high)
        tail = jnp.sum(tail[:count] + tail[count:], axis=1, keepdims=True)
        spread = one_hot.astype(high) * tail
        spread_high = spread.astype(low)
        spread_low = (spread - spread_high.astype(high)).astype(low)
        group = (
            lax.broadcasted_iota(jnp.int32, (count, experts), 0) // slots
            == lax.broadcasted_iota(jnp.int32, (count, experts), 1)
        ).astype(low)
        items = [
            dot(spread_high, group, ((0,), (0,))),
            dot(spread_low, group, ((0,), (0,))),
        ]
        score = sum(items) if score is None else score + sum(items)
        both = dot(one_hot, home[:count, :width], ((0,), (0,)))
        both = both + dot(one_hot, home[count:, :width], ((0,), (0,)))
        total = both if total is None else total + both
    grad_logits = (
        score - gates[...] * jnp.sum(score, axis=1, keepdims=True)
    ).astype(low)
    grad_normed = total + dot(grad_logits, router_weight[...], ((1,), (1,)))
    widened = tokens[...].astype(high)
    inverse = lax.rsqrt(jnp.mean(widened * widened, axis=1, keepdims=True) + EPSILON)
    scaled = widened * inverse
    gained = (scaled * norm_gain[...]).astype(low)
    gain = grad_normed * scaled
    gain_high = gain.astype(low)
    gain_low = (gain - gain_high.astype(high)).astype(low)
    ones = jnp.ones((gain.shape[0], experts), low)
    gain_sum = dot(gain_high, ones, ((0,), (0,))) + dot(gain_low, ones, ((0,), (0,)))
    lane = lax.broadcasted_iota(jnp.int32, gain_sum.shape, 1)
    sum_high = gain_sum.astype(low).astype(high)
    gain_parts = jnp.where(lane == 0, sum_high, jnp.where(lane == 1, gain_sum - sum_high, 0.0))
    router_part = dot(gained, grad_logits, ((0,), (0,)))
    part = jnp.concatenate([router_part, gain_parts], axis=1).astype(low)
    part_sums[...] = part.reshape(part_sums.shape)
    grad_scaled = grad_normed * norm_gain[...]
    correction = jnp.mean(grad_scaled * scaled, axis=1, keepdims=True)
    grad_tokens[...] = (
        cotangent[...].astype(high) + inverse * (grad_scaled - scaled * correction)
    ).astype(low)

    pairs = part_sums.shape[0] // DEVICES

    def piece(k):
        dp, ctx = target(k)
        return remote(
            part_sums.at[pl.ds((dp * 32 + ctx) * pairs, pairs)], all_sums.at[k],
            sum_send.at[k], sum_recv.at[k], (dp, ctx),
        )

    def piece_go(k, carry):
        piece(k).start()
        return carry

    lax.fori_loop(1, DEVICES, piece_go, 0)
    all_sums[0] = part_sums[pl.ds((mine[0] * 32 + mine[1]) * pairs, pairs)]

    def drain(k, carry):
        go_main(k).wait_send()
        go_extra(k).wait_send()
        for kind in range(2):
            home_copy(k, source(k), own_index, kind).wait_send()
        return carry

    lax.fori_loop(1, DEVICES, drain, 0)
    for item in moves:
        item.wait()

    def piece_came(k, carry):
        piece(k).wait()
        return carry

    lax.fori_loop(1, DEVICES, piece_came, 0)
    sums[...] = jnp.sum(all_sums[...].astype(high), axis=0)


TILE = 256


def moe(out_main, out_extra, weights, local):
    half, width = weights[2].shape[1:]
    units = 2 * half
    count = DEVICES * (SLOTS + EXTRA)
    low = jnp.bfloat16
    anywhere = pl.BlockSpec(memory_space=pl.ANY)
    pair = pltpu.SemaphoreType.DMA((2, DEVICES))
    three = pltpu.SemaphoreType.DMA((3,))
    each = pltpu.SemaphoreType.DMA((DEVICES,))
    vmem = pl.BlockSpec(memory_space=pltpu.VMEM)
    pairs = width // (2 * DEVICES)
    return pl.pallas_call(
        moe_kernel,
        out_shape=[
            jax.ShapeDtypeStruct(local[3].shape, low),
            jax.ShapeDtypeStruct((2, width, half), low),
            jax.ShapeDtypeStruct((2, width, half), low),
            jax.ShapeDtypeStruct((2, half, width), low),
            jax.ShapeDtypeStruct((pairs, 2, 128), jnp.float32),
            jax.ShapeDtypeStruct((2 * SLOTS, width + 128), low),
        ],
        in_specs=[anywhere] * 5 + [vmem] * 7,
        out_specs=[vmem] + [anywhere] * 3 + [vmem, anywhere],
        scratch_shapes=[
            pltpu.VMEM((DEVICES * SLOTS, width + 128), low),
            pltpu.VMEM((DEVICES * EXTRA, width + 128), low),
            pltpu.VMEM((DEVICES * pairs, 2, 128), low),
            pltpu.VMEM((DEVICES, pairs, 2, 128), low),
            pltpu.VMEM((count, 2 * width), low),
            pltpu.VMEM((count, width + 128), low),
            pltpu.VMEM((width, units), low),
            pltpu.VMEM((width, units), low),
            pltpu.VMEM((units, width), low),
            pltpu.VMEM((count, units), low),
            pltpu.VMEM((count, units), low),
            pltpu.VMEM((count, units), low),
            pltpu.VMEM((width, units), low),
            pltpu.VMEM((width, units), low),
            pltpu.VMEM((units, width), low),
            pair, pair, pair, pair,
            pltpu.SemaphoreType.DMA((2,)),
            three, three, three, three, three,
            each, each,
        ],
        compiler_params=pltpu.CompilerParams(
            collective_id=1, has_side_effects=True, vmem_limit_bytes=60 * 2**20
        ),
    )(out_main, out_extra, *weights, *local)


def body(
    tokens, cotangent, expert_ids, norm_gain, router_weight, gate_weight, up_weight, down_weight
):
    experts = router_weight.shape[1]
    rows_here, width = tokens.shape
    widened = tokens.astype(jnp.float32)
    inverse = lax.rsqrt(jnp.mean(widened * widened, axis=1, keepdims=True) + EPSILON)
    scaled = widened * inverse
    normed = (scaled * norm_gain).astype(jnp.bfloat16)
    logits = jnp.dot(normed, router_weight, preferred_element_type=jnp.float32)
    labels = jnp.arange(experts, dtype=jnp.int32)
    member = jnp.any(expert_ids[:, :, None] == labels, axis=1)
    lifted = jnp.where(member, jnp.exp(jnp.where(member, logits, 0.0)), 0.0)
    gates = lifted / jnp.sum(lifted, axis=1, keepdims=True)
    earlier = (
        jnp.arange(rows_here)[:, None] > jnp.arange(rows_here)[None, :]
    ).astype(jnp.bfloat16)
    rank = jnp.dot(earlier, member.astype(jnp.bfloat16), preferred_element_type=jnp.float32)
    rank = jnp.where(member, rank, -1.0).T

    def slots_of(first, count):
        block = jnp.repeat(rank, count, axis=0)
        slot = jnp.arange(experts * count, dtype=jnp.int32) % count + first
        return block == slot.astype(jnp.float32)[:, None]

    both = jnp.concatenate([normed, cotangent], axis=1)

    def dispatched(pick, slots):
        gate = jnp.sum(jnp.where(pick, jnp.repeat(gates.T, slots, axis=0), 0.0), axis=1)
        moved = jnp.dot(pick.astype(jnp.bfloat16), both, preferred_element_type=jnp.float32)
        is_upstream = jnp.arange(2 * width) >= width
        moved = moved * jnp.where(is_upstream[None, :], gate[:, None], 1.0)
        return moved.astype(jnp.bfloat16)

    picks = [slots_of(0, SLOTS), slots_of(SLOTS, EXTRA)]
    out_main = dispatched(picks[0], SLOTS)
    out_extra = dispatched(picks[1], EXTRA)
    picks = [pick.astype(jnp.bfloat16) for pick in picks]

    grad_tokens, *grads, sums, _ = moe(
        out_main,
        out_extra,
        (gate_weight, up_weight, down_weight),
        (*picks, gates, tokens, cotangent, norm_gain[None, :], router_weight),
    )
    sums = sums.reshape(width // DEVICES, 128)
    return (grad_tokens, *grads, sums[:, :experts], sums[:, experts] + sums[:, experts + 1])


def solution(mesh):
    return jax.shard_map(
        body,
        mesh=mesh,
        in_specs=(
            P(("dp", "ctx"), None),
            P(("dp", "ctx"), None),
            P(("dp", "ctx"), None),
            P(),
            P(),
            P("ctx", None, "dp"),
            P("ctx", None, "dp"),
            P("ctx", "dp", None),
        ),
        out_specs=(
            P(("dp", "ctx"), None),
            P("ctx", None, "dp"),
            P("ctx", None, "dp"),
            P("ctx", "dp", None),
            P(("dp", "ctx"), None),
            P(("dp", "ctx")),
        ),
        check_vma=False,
    )
```

```python
import functools

import jax
import jax.numpy as jnp
from jax import lax
from jax.experimental import pallas as pl
from jax.experimental.pallas import tpu as pltpu
from jax.sharding import PartitionSpec as P

EPSILON = 1e-05
SWISH_SCALE = 1.702
MESH = pl.DeviceIdType.MESH
SLOTS = 8
EXTRA = 2
ROW_BLOCK = 256
DEVICES = 128


def coordinates():
    dp, ctx = lax.axis_index("dp"), lax.axis_index("ctx")
    return (ctx // 4) % 4, ctx % 4, (dp // 2) * 2 + ctx // 16, dp % 2


def device_of(x, y, z, core):
    return (z // 2) * 2 + core, (z % 2) * 16 + x * 4 + y


def expert_of(dp, ctx):
    return 2 * ctx + dp % 2


def half_and_expert(dp, ctx):
    return (dp // 2) * 64 + expert_of(dp, ctx)


def dot(a, b, contract):
    return lax.dot_general(a, b, (contract, ((), ())), preferred_element_type=jnp.float32)


def moe_kernel(
    gate_weight, up_weight, down_weight,
    tokens, cotangent, expert_ids, norm_gain, router_weight,
    grad_tokens, gate_grad, up_grad, down_grad, sums, bounce,
    out_main, out_extra, pick_main, pick_extra, gates, home_main, home_extra, part_sums, all_sums, rows, back, w_gate, w_up, w_down, hid, gat, upp, gate_buf, up_buf, down_buf,
    go_send, go_recv, home_send, home_recv, local_sem, load_sem,
    weight_send, weight_recv, grad_send, grad_recv, sum_send, sum_recv,
):
    x, y, z, core = coordinates()
    mine = device_of(x, y, z, core)
    partner = device_of(x, y, z, 1 - core)
    edge = DEVICES * SLOTS
    half = down_weight.shape[1]
    width = down_weight.shape[2]

    def turn(k, sign, flip):
        return device_of(
            (x + sign * k + DEVICES) % 4,
            (y + sign * (3 * k + k // 4) + 4 * DEVICES) % 4,
            (z + sign * (2 * k + k // 4 + k // 16) + 4 * DEVICES) % 4,
            flip,
        )

    def target(k):
        return turn(k, 1 - 2 * core, (core + k // 64 + k // 4) % 2)

    def source(k):
        other = (core + k // 64 + k // 4) % 2
        return turn(k, 2 * other - 1, other)

    def main_slot(ref, i):
        return ref.at[pl.ds(pl.multiple_of(i * SLOTS, SLOTS), SLOTS)]

    def extra_slot(ref, i, first=0):
        return ref.at[pl.ds(pl.multiple_of(first + i * EXTRA, EXTRA), EXTRA)]

    barrier = pltpu.get_barrier_semaphore()

    def greet(k, carry):
        pl.semaphore_signal(barrier, inc=1, device_id=target(k), device_id_type=MESH)
        return carry

    lax.fori_loop(1, DEVICES, greet, 0)

    low, high = jnp.bfloat16, jnp.float32
    experts = router_weight.shape[1]
    tokens_here = tokens.shape[0]
    places = (w_gate, w_up, w_down)

    def part(buf, i):
        at = pl.ds(i * half, half)
        return buf.at[at] if buf.shape[0] == 2 * half else buf.at[:, at]

    loads = [
        pltpu.make_async_copy(weight.at[core], part(place, 0), load_sem.at[i])
        for i, (weight, place) in enumerate(zip((gate_weight, up_weight, down_weight), places))
    ]
    for item in loads:
        item.start()

    def iota(shape, dim):
        return lax.broadcasted_iota(jnp.int32, shape, dim)

    def normalized():
        widened = tokens[...].astype(high)
        inverse = lax.rsqrt(jnp.mean(widened * widened, axis=1, keepdims=True) + EPSILON)
        scaled = widened * inverse
        return inverse, scaled, (scaled * norm_gain[...]).astype(low)

    normed_here = normalized()[2]
    logits = dot(normed_here, router_weight[...], ((1,), (0,)))
    label = iota((tokens_here, experts), 1)
    ids = expert_ids[...]
    member = ids[:, 0:1] == label
    for k in range(1, ids.shape[1]):
        member = member | (ids[:, k : k + 1] == label)
    lifted = jnp.where(member, jnp.exp(jnp.where(member, logits, 0.0)), 0.0)
    gate = lifted / jnp.sum(lifted, axis=1, keepdims=True)
    gates[...] = gate
    gate_high = gate.astype(low)
    gate_low = (gate - gate_high.astype(high)).astype(low)
    earlier = iota((tokens_here, tokens_here), 0) > iota((tokens_here, tokens_here), 1)
    named = member.astype(high).astype(low)
    rank = dot(earlier.astype(high).astype(low), named, ((1,), (0,)))
    rank = jnp.where(member, rank, -1.0).astype(low)
    for out, chosen, slots, first in (
        (out_main, pick_main, SLOTS, 0), (out_extra, pick_extra, EXTRA, SLOTS)
    ):
        count = experts * slots
        spread = (iota((experts, count), 1) // slots == iota((experts, count), 0))
        spread = spread.astype(high).astype(low)
        slot = (iota((tokens_here, count), 1) % slots + first).astype(high)
        hit = dot(rank, spread, ((1,), (0,))) == slot
        one_hot = hit.astype(high).astype(low)
        chosen[...] = one_hot
        out[:, :width] = dot(one_hot, normed_here, ((0,), (0,))).astype(low)
        scaled_up = None
        for piece_of in (gate_high, gate_low):
            weighted = jnp.where(hit, dot(piece_of, spread, ((1,), (0,))), 0.0).astype(low)
            term = dot(weighted, cotangent[...], ((0,), (0,)))
            scaled_up = term if scaled_up is None else scaled_up + term
        out[:, width:] = scaled_up.astype(low)

    pl.semaphore_wait(barrier, DEVICES - 1)

    def remote(src, dst, send, recv, device):
        return pltpu.make_async_remote_copy(
            src_ref=src, dst_ref=dst, send_sem=send, recv_sem=recv,
            device_id=device, device_id_type=MESH,
        )

    def go_main(k):
        to = target(k)
        return remote(
            main_slot(out_main, expert_of(*to)), main_slot(rows, k),
            go_send.at[0, k], go_recv.at[0, k], to,
        )

    def go_extra(k):
        to = target(k)
        return remote(
            extra_slot(out_extra, expert_of(*to)), extra_slot(rows, k, edge),
            go_send.at[1, k], go_recv.at[1, k], to,
        )

    def home_copy(k, to, index, kind):
        if kind == 0:
            src, dst = main_slot(back, k), main_slot(home_main, index)
        else:
            src, dst = extra_slot(back, k, edge), extra_slot(home_extra, index)
        return remote(src, dst, home_send.at[kind, k], home_recv.at[kind, index], to)

    own_index = half_and_expert(*mine)

    def return_main(k, carry):
        home_copy(k, source(k), own_index, 0).start()
        return carry

    def return_extra(k, carry):
        home_copy(k, source(k), own_index, 1).start()
        return carry

    swaps = [
        remote(weight.at[1 - core], part(place, 1), weight_send.at[i], weight_recv.at[i], partner)
        for i, (weight, place) in enumerate(zip((gate_weight, up_weight, down_weight), places))
    ]
    own = expert_of(*mine)
    leave = [
        pltpu.make_async_copy(main_slot(out_main, own), main_slot(bounce, 0), local_sem.at[0]),
        pltpu.make_async_copy(extra_slot(out_extra, own), extra_slot(bounce, 0, SLOTS), local_sem.at[1]),
    ]
    enter = [
        pltpu.make_async_copy(main_slot(bounce, 0), main_slot(rows, 0), local_sem.at[0]),
        pltpu.make_async_copy(
            extra_slot(bounce, 0, SLOTS), extra_slot(rows, 0, edge), local_sem.at[1]
        ),
    ]

    def go(k, carry):
        go_main(k).start()
        go_extra(k).start()
        return carry

    lax.fori_loop(1, DEVICES, go, 0)
    for item in swaps + leave:
        item.start()
    for item in leave:
        item.wait()
    for item in enter:
        item.start()
    for item in loads + swaps + enter:
        item.wait()

    def main_came(k, carry):
        go_main(k).wait_recv()
        return carry

    def extra_came(k, carry):
        go_extra(k).wait_recv()
        return carry

    senders = ROW_BLOCK // SLOTS
    blocks = edge // ROW_BLOCK

    def step(i, carry):
        first = i * senders
        lax.fori_loop(jnp.maximum(first, 1), jnp.minimum(first + senders, DEVICES), main_came, 0)
        lax.fori_loop(DEVICES - (i // blocks) * (DEVICES - 1), DEVICES, extra_came, 0)
        block = pl.ds(pl.multiple_of(i * ROW_BLOCK, ROW_BLOCK), ROW_BLOCK)
        normed = rows[block, :width]
        upstream = rows[block, width:]
        gate_pre = dot(normed, w_gate[...], ((1,), (0,)))
        up_pre = dot(normed, w_up[...], ((1,), (0,))) + 1.0
        grad_hidden = dot(upstream, w_down[...], ((1,), (1,)))
        squash = jax.nn.sigmoid(SWISH_SCALE * gate_pre)
        swish = gate_pre * squash
        hidden = (swish * up_pre).astype(jnp.bfloat16)
        slope = squash + SWISH_SCALE * swish * (1.0 - squash)
        pre_gate = (grad_hidden * up_pre * slope).astype(jnp.bfloat16)
        pre_up = (grad_hidden * swish).astype(jnp.bfloat16)
        hid[block, :] = hidden
        gat[block, :] = pre_gate
        upp[block, :] = pre_up
        score = jnp.sum(grad_hidden * hidden.astype(jnp.float32), axis=1, keepdims=True)
        high = score.astype(jnp.bfloat16).astype(jnp.float32)
        lane = lax.broadcasted_iota(jnp.int32, (ROW_BLOCK, 128), 1)
        tail = jnp.where(lane == 0, high, jnp.where(lane == 1, score - high, 0.0))
        total = dot(pre_gate, w_gate[...], ((1,), (1,))) + dot(pre_up, w_up[...], ((1,), (1,)))
        back[block, :width] = total.astype(jnp.bfloat16)
        back[block, width:] = tail.astype(jnp.bfloat16)
        lax.fori_loop(jnp.maximum(first - senders, 1), first, return_main, 0)
        return carry

    lax.fori_loop(0, blocks + 1, step, 0)

    def columns(i, carry):
        at = pl.ds(pl.multiple_of(i * TILE, TILE), TILE)
        tile = rows[:, at]
        gate_buf[at, :] = dot(tile, gat[...], ((0,), (0,))).astype(jnp.bfloat16)
        up_buf[at, :] = dot(tile, upp[...], ((0,), (0,))).astype(jnp.bfloat16)
        return carry

    def units(i, carry):
        at = pl.ds(pl.multiple_of(i * TILE, TILE), TILE)
        down_buf[at, :] = dot(hid[:, at], rows[:, width:], ((0,), (0,))).astype(jnp.bfloat16)
        return carry

    lax.fori_loop(0, 1, units, 0)
    lax.fori_loop(1, DEVICES, return_extra, 0)
    lanes = back.shape[1]
    near = bounce.at[:, pl.ds(0, lanes)]
    away = [
        pltpu.make_async_copy(main_slot(back, 0), main_slot(near, 0), local_sem.at[0]),
        pltpu.make_async_copy(extra_slot(back, 0, edge), extra_slot(near, 0, SLOTS), local_sem.at[1]),
    ]
    kept = [
        pltpu.make_async_copy(main_slot(near, 0), main_slot(home_main, own_index), local_sem.at[0]),
        pltpu.make_async_copy(
            extra_slot(near, 0, SLOTS), extra_slot(home_extra, own_index), local_sem.at[1]
        ),
    ]
    for item in away:
        item.start()
    lax.fori_loop(1, 2 * half // TILE, units, 0)
    for item in away:
        item.wait()
    for item in kept:
        item.start()
    lax.fori_loop(0, width // TILE, columns, 0)
    grads = zip((down_buf, gate_buf, up_buf), (down_grad, gate_grad, up_grad))
    moves = []
    for i, (buf, out) in enumerate(grads):
        moves.append(remote(part(buf, 1), out.at[core], grad_send.at[i], grad_recv.at[i], partner))
        moves.append(pltpu.make_async_copy(part(buf, 0), out.at[core], load_sem.at[i]))
    for item in moves:
        item.start()

    def home_came(k, carry):
        index = half_and_expert(*target(k))
        for kind in range(2):
            home_copy(k, source(k), index, kind).wait_recv()
        return carry

    lax.fori_loop(1, DEVICES, home_came, 0)
    for item in kept:
        item.wait()

    total, score = None, None
    for pick, home, slots in ((pick_main, home_main, SLOTS), (pick_extra, home_extra, EXTRA)):
        count = experts * slots
        one_hot = pick[...]
        tail = home[:, width:].astype(high)
        tail = jnp.sum(tail[:count] + tail[count:], axis=1, keepdims=True)
        group = iota((count, experts), 0) // slots == iota((count, experts), 1)
        spread = jnp.where(group, tail, 0.0)
        spread_high = spread.astype(low)
        spread_low = (spread - spread_high.astype(high)).astype(low)
        here = dot(one_hot, spread_high, ((1,), (0,))) + dot(one_hot, spread_low, ((1,), (0,)))
        score = here if score is None else score + here
        both = dot(one_hot, home[:count, :width], ((1,), (0,)))
        both = both + dot(one_hot, home[count:, :width], ((1,), (0,)))
        total = both if total is None else total + both
    grad_logits = (
        score - gates[...] * jnp.sum(score, axis=1, keepdims=True)
    ).astype(low)
    grad_normed = total + dot(grad_logits, router_weight[...], ((1,), (1,)))
    inverse, scaled, gained = normalized()
    gain = grad_normed * scaled
    gain_high = gain.astype(low)
    gain_low = (gain - gain_high.astype(high)).astype(low)
    ones = jnp.ones((gain.shape[0], experts), low)
    gain_sum = dot(gain_high, ones, ((0,), (0,))) + dot(gain_low, ones, ((0,), (0,)))
    lane = iota(gain_sum.shape, 1)
    sum_high = gain_sum.astype(low).astype(high)
    gain_parts = jnp.where(lane == 0, sum_high, jnp.where(lane == 1, gain_sum - sum_high, 0.0))
    router_part = dot(gained, grad_logits, ((0,), (0,)))
    part = jnp.concatenate([router_part, gain_parts], axis=1).astype(low)
    part_sums[...] = part.reshape(part_sums.shape)
    grad_scaled = grad_normed * norm_gain[...]
    correction = jnp.mean(grad_scaled * scaled, axis=1, keepdims=True)
    grad_tokens[...] = (
        cotangent[...].astype(high) + inverse * (grad_scaled - scaled * correction)
    ).astype(low)

    pairs = part_sums.shape[0] // DEVICES

    def piece(k):
        dp, ctx = target(k)
        return remote(
            part_sums.at[pl.ds((dp * 32 + ctx) * pairs, pairs)], all_sums.at[k],
            sum_send.at[k], sum_recv.at[k], (dp, ctx),
        )

    def piece_go(k, carry):
        piece(k).start()
        return carry

    lax.fori_loop(1, DEVICES, piece_go, 0)
    all_sums[0] = part_sums[pl.ds((mine[0] * 32 + mine[1]) * pairs, pairs)]

    def drain(k, carry):
        go_main(k).wait_send()
        go_extra(k).wait_send()
        for kind in range(2):
            home_copy(k, source(k), own_index, kind).wait_send()
        return carry

    lax.fori_loop(1, DEVICES, drain, 0)
    for item in moves:
        item.wait()

    def piece_came(k, carry):
        piece(k).wait()
        return carry

    lax.fori_loop(1, DEVICES, piece_came, 0)
    sums[...] = jnp.sum(all_sums[...].astype(high), axis=0)


TILE = 256


def moe(weights, local):
    half, width = weights[2].shape[1:]
    units = 2 * half
    count = DEVICES * (SLOTS + EXTRA)
    low = jnp.bfloat16
    anywhere = pl.BlockSpec(memory_space=pl.ANY)
    pair = pltpu.SemaphoreType.DMA((2, DEVICES))
    three = pltpu.SemaphoreType.DMA((3,))
    each = pltpu.SemaphoreType.DMA((DEVICES,))
    vmem = pl.BlockSpec(memory_space=pltpu.VMEM)
    pairs = width // (2 * DEVICES)
    here, experts = local[0].shape[0], local[4].shape[1]
    return pl.pallas_call(
        moe_kernel,
        out_shape=[
            jax.ShapeDtypeStruct(local[0].shape, low),
            jax.ShapeDtypeStruct((2, width, half), low),
            jax.ShapeDtypeStruct((2, width, half), low),
            jax.ShapeDtypeStruct((2, half, width), low),
            jax.ShapeDtypeStruct((pairs, 2, 128), jnp.float32),
            jax.ShapeDtypeStruct((2 * SLOTS, 2 * width), low),
        ],
        in_specs=[anywhere] * 3 + [vmem] * 5,
        out_specs=[vmem] + [anywhere] * 3 + [vmem, anywhere],
        scratch_shapes=[
            pltpu.VMEM((experts * SLOTS, 2 * width), low),
            pltpu.VMEM((experts * EXTRA, 2 * width), low),
            pltpu.VMEM((here, experts * SLOTS), low),
            pltpu.VMEM((here, experts * EXTRA), low),
            pltpu.VMEM((here, experts), jnp.float32),
            pltpu.VMEM((DEVICES * SLOTS, width + 128), low),
            pltpu.VMEM((DEVICES * EXTRA, width + 128), low),
            pltpu.VMEM((DEVICES * pairs, 2, 128), low),
            pltpu.VMEM((DEVICES, pairs, 2, 128), low),
            pltpu.VMEM((count, 2 * width), low),
            pltpu.VMEM((count, width + 128), low),
            pltpu.VMEM((width, units), low),
            pltpu.VMEM((width, units), low),
            pltpu.VMEM((units, width), low),
            pltpu.VMEM((count, units), low),
            pltpu.VMEM((count, units), low),
            pltpu.VMEM((count, units), low),
            pltpu.VMEM((width, units), low),
            pltpu.VMEM((width, units), low),
            pltpu.VMEM((units, width), low),
            pair, pair, pair, pair,
            pltpu.SemaphoreType.DMA((2,)),
            three, three, three, three, three,
            each, each,
        ],
        compiler_params=pltpu.CompilerParams(
            collective_id=1, has_side_effects=True, vmem_limit_bytes=60 * 2**20
        ),
    )(*weights, *local)


def body(
    tokens, cotangent, expert_ids, norm_gain, router_weight, gate_weight, up_weight, down_weight
):
    experts = router_weight.shape[1]
    width = tokens.shape[1]
    grad_tokens, *grads, sums, _ = moe(
        (gate_weight, up_weight, down_weight),
        (tokens, cotangent, expert_ids, norm_gain[None, :], router_weight),
    )
    sums = sums.reshape(width // DEVICES, 128)
    return (grad_tokens, *grads, sums[:, :experts], sums[:, experts] + sums[:, experts + 1])


def solution(mesh):
    return jax.shard_map(
        body,
        mesh=mesh,
        in_specs=(
            P(("dp", "ctx"), None),
            P(("dp", "ctx"), None),
            P(("dp", "ctx"), None),
            P(),
            P(),
            P("ctx", None, "dp"),
            P("ctx", None, "dp"),
            P("ctx", "dp", None),
        ),
        out_specs=(
            P(("dp", "ctx"), None),
            P("ctx", None, "dp"),
            P("ctx", None, "dp"),
            P("ctx", "dp", None),
            P(("dp", "ctx"), None),
            P(("dp", "ctx")),
        ),
        check_vma=False,
    )
```

```python
import functools

import jax
import jax.numpy as jnp
from jax import lax
from jax.experimental import pallas as pl
from jax.experimental.pallas import tpu as pltpu
from jax.sharding import PartitionSpec as P

EPSILON = 1e-05
SWISH_SCALE = 1.702
MESH = pl.DeviceIdType.MESH
SLOTS = 8
EXTRA = 2
ROW_BLOCK = 256
DEVICES = 128


def coordinates():
    dp, ctx = lax.axis_index("dp"), lax.axis_index("ctx")
    return (ctx // 4) % 4, ctx % 4, (dp // 2) * 2 + ctx // 16, dp % 2


def device_of(x, y, z, core):
    return (z // 2) * 2 + core, (z % 2) * 16 + x * 4 + y


def expert_of(dp, ctx):
    return 2 * ctx + dp % 2


def half_and_expert(dp, ctx):
    return (dp // 2) * 64 + expert_of(dp, ctx)


def dot(a, b, contract):
    return lax.dot_general(a, b, (contract, ((), ())), preferred_element_type=jnp.float32)


def moe_kernel(
    gate_weight, up_weight, down_weight,
    tokens, cotangent, expert_ids, norm_gain, router_weight,
    grad_tokens, gate_grad, up_grad, down_grad, sums, bounce,
    out_main, out_extra, pick_main, pick_extra, gates, home_main, home_extra, part_sums, all_sums, rows, back, w_gate, w_up, w_down, hid, gat, upp, gate_buf, up_buf, down_buf,
    go_send, go_recv, home_send, home_recv, local_sem, load_sem,
    weight_send, weight_recv, grad_send, grad_recv, sum_send, sum_recv,
):
    x, y, z, core = coordinates()
    mine = device_of(x, y, z, core)
    partner = device_of(x, y, z, 1 - core)
    edge = DEVICES * SLOTS
    half = down_weight.shape[1]
    width = down_weight.shape[2]

    def turn(k, sign, flip):
        return device_of(
            (x + sign * k + DEVICES) % 4,
            (y + sign * (3 * k + k // 4) + 4 * DEVICES) % 4,
            (z + sign * (2 * k + k // 4 + k // 16) + 4 * DEVICES) % 4,
            flip,
        )

    def target(k):
        return turn(k, 1 - 2 * core, (core + k // 64 + k // 4) % 2)

    def source(k):
        other = (core + k // 64 + k // 4) % 2
        return turn(k, 2 * other - 1, other)

    def main_slot(ref, i):
        return ref.at[pl.ds(pl.multiple_of(i * SLOTS, SLOTS), SLOTS)]

    def extra_slot(ref, i, first=0):
        return ref.at[pl.ds(pl.multiple_of(first + i * EXTRA, EXTRA), EXTRA)]

    barrier = pltpu.get_barrier_semaphore()

    def greet(k, carry):
        pl.semaphore_signal(barrier, inc=1, device_id=target(k), device_id_type=MESH)
        return carry

    lax.fori_loop(1, DEVICES, greet, 0)

    low, high = jnp.bfloat16, jnp.float32
    experts = router_weight.shape[0]
    tokens_here = tokens.shape[0]
    places = (w_gate, w_up, w_down)

    def part(buf, i):
        at = pl.ds(i * half, half)
        return buf.at[at] if buf.shape[0] == 2 * half else buf.at[:, at]

    loads = [
        pltpu.make_async_copy(weight.at[core], part(place, 0), load_sem.at[i])
        for i, (weight, place) in enumerate(zip((gate_weight, up_weight, down_weight), places))
    ]
    for item in loads:
        item.start()

    def iota(shape, dim):
        return lax.broadcasted_iota(jnp.int32, shape, dim)

    def as_low(flag):
        return flag.astype(high).astype(low)

    gain_row = jnp.concatenate([norm_gain[i : i + 1, :] for i in range(width // 128)], axis=1)

    def normalized():
        widened = tokens[...].astype(high)
        inverse = lax.rsqrt(jnp.mean(widened * widened, axis=1, keepdims=True) + EPSILON)
        scaled = widened * inverse
        return inverse, scaled, (scaled * gain_row).astype(low)

    normed_here = normalized()[2]
    logits = dot(normed_here, router_weight[...], ((1,), (1,)))
    label = iota((experts, tokens_here), 0)
    ids = expert_ids[...]
    turned = ids[0:1] == label
    for k in range(1, ids.shape[0]):
        turned = turned | (ids[k : k + 1] == label)
    same = iota((experts, experts), 0) == iota((experts, experts), 1)
    member = dot(as_low(turned), as_low(same), ((0,), (0,))) > 0.5
    lifted = jnp.where(member, jnp.exp(jnp.where(member, logits, 0.0)), 0.0)
    gate = lifted / jnp.sum(lifted, axis=1, keepdims=True)
    gates[...] = gate
    gate_high = gate.astype(low)
    gate_low = (gate - gate_high.astype(high)).astype(low)
    earlier = iota((tokens_here, tokens_here), 0) > iota((tokens_here, tokens_here), 1)
    named = as_low(member)
    rank = dot(as_low(earlier), named, ((1,), (0,)))
    rank = jnp.where(member, rank, -1.0).astype(low)
    for out, chosen, slots, first in (
        (out_main, pick_main, SLOTS, 0), (out_extra, pick_extra, EXTRA, SLOTS)
    ):
        count = experts * slots
        spread = (iota((experts, count), 1) // slots == iota((experts, count), 0))
        spread = as_low(spread)
        slot = (iota((tokens_here, count), 1) % slots + first).astype(high)
        hit = dot(rank, spread, ((1,), (0,))) == slot
        one_hot = as_low(hit)
        chosen[...] = one_hot
        out[:, :width] = dot(one_hot, normed_here, ((0,), (0,))).astype(low)
        scaled_up = None
        for piece_of in (gate_high, gate_low):
            weighted = jnp.where(hit, dot(piece_of, spread, ((1,), (0,))), 0.0).astype(low)
            term = dot(weighted, cotangent[...], ((0,), (0,)))
            scaled_up = term if scaled_up is None else scaled_up + term
        out[:, width:] = scaled_up.astype(low)

    pl.semaphore_wait(barrier, DEVICES - 1)

    def remote(src, dst, send, recv, device):
        return pltpu.make_async_remote_copy(
            src_ref=src, dst_ref=dst, send_sem=send, recv_sem=recv,
            device_id=device, device_id_type=MESH,
        )

    def go_main(k):
        to = target(k)
        return remote(
            main_slot(out_main, expert_of(*to)), main_slot(rows, k),
            go_send.at[0, k], go_recv.at[0, k], to,
        )

    def go_extra(k):
        to = target(k)
        return remote(
            extra_slot(out_extra, expert_of(*to)), extra_slot(rows, k, edge),
            go_send.at[1, k], go_recv.at[1, k], to,
        )

    def home_copy(k, to, index, kind):
        if kind == 0:
            src, dst = main_slot(back, k), main_slot(home_main, index)
        else:
            src, dst = extra_slot(back, k, edge), extra_slot(home_extra, index)
        return remote(src, dst, home_send.at[kind, k], home_recv.at[kind, index], to)

    own_index = half_and_expert(*mine)

    def return_main(k, carry):
        home_copy(k, source(k), own_index, 0).start()
        return carry

    def return_extra(k, carry):
        home_copy(k, source(k), own_index, 1).start()
        return carry

    swaps = [
        remote(weight.at[1 - core], part(place, 1), weight_send.at[i], weight_recv.at[i], partner)
        for i, (weight, place) in enumerate(zip((gate_weight, up_weight, down_weight), places))
    ]
    own = expert_of(*mine)
    leave = [
        pltpu.make_async_copy(main_slot(out_main, own), main_slot(bounce, 0), local_sem.at[0]),
        pltpu.make_async_copy(extra_slot(out_extra, own), extra_slot(bounce, 0, SLOTS), local_sem.at[1]),
    ]
    enter = [
        pltpu.make_async_copy(main_slot(bounce, 0), main_slot(rows, 0), local_sem.at[0]),
        pltpu.make_async_copy(
            extra_slot(bounce, 0, SLOTS), extra_slot(rows, 0, edge), local_sem.at[1]
        ),
    ]

    def go(k, carry):
        go_main(k).start()
        go_extra(k).start()
        return carry

    lax.fori_loop(1, DEVICES, go, 0)
    for item in swaps + leave:
        item.start()
    for item in leave:
        item.wait()
    for item in enter:
        item.start()
    for item in loads + swaps + enter:
        item.wait()

    def main_came(k, carry):
        go_main(k).wait_recv()
        return carry

    def extra_came(k, carry):
        go_extra(k).wait_recv()
        return carry

    senders = ROW_BLOCK // SLOTS
    blocks = edge // ROW_BLOCK

    def step(i, carry):
        first = i * senders
        lax.fori_loop(jnp.maximum(first, 1), jnp.minimum(first + senders, DEVICES), main_came, 0)
        lax.fori_loop(DEVICES - (i // blocks) * (DEVICES - 1), DEVICES, extra_came, 0)
        block = pl.ds(pl.multiple_of(i * ROW_BLOCK, ROW_BLOCK), ROW_BLOCK)
        normed = rows[block, :width]
        upstream = rows[block, width:]
        gate_pre = dot(normed, w_gate[...], ((1,), (0,)))
        up_pre = dot(normed, w_up[...], ((1,), (0,))) + 1.0
        grad_hidden = dot(upstream, w_down[...], ((1,), (1,)))
        squash = jax.nn.sigmoid(SWISH_SCALE * gate_pre)
        swish = gate_pre * squash
        hidden = (swish * up_pre).astype(jnp.bfloat16)
        slope = squash + SWISH_SCALE * swish * (1.0 - squash)
        pre_gate = (grad_hidden * up_pre * slope).astype(jnp.bfloat16)
        pre_up = (grad_hidden * swish).astype(jnp.bfloat16)
        hid[block, :] = hidden
        gat[block, :] = pre_gate
        upp[block, :] = pre_up
        score = jnp.sum(grad_hidden * hidden.astype(jnp.float32), axis=1, keepdims=True)
        high = score.astype(jnp.bfloat16).astype(jnp.float32)
        lane = lax.broadcasted_iota(jnp.int32, (ROW_BLOCK, 128), 1)
        tail = jnp.where(lane == 0, high, jnp.where(lane == 1, score - high, 0.0))
        total = dot(pre_gate, w_gate[...], ((1,), (1,))) + dot(pre_up, w_up[...], ((1,), (1,)))
        back[block, :width] = total.astype(jnp.bfloat16)
        back[block, width:] = tail.astype(jnp.bfloat16)
        lax.fori_loop(jnp.maximum(first - senders, 1), first, return_main, 0)
        return carry

    lax.fori_loop(0, blocks + 1, step, 0)

    def columns(i, carry):
        at = pl.ds(pl.multiple_of(i * TILE, TILE), TILE)
        tile = rows[:, at]
        gate_buf[at, :] = dot(tile, gat[...], ((0,), (0,))).astype(jnp.bfloat16)
        up_buf[at, :] = dot(tile, upp[...], ((0,), (0,))).astype(jnp.bfloat16)
        return carry

    def units(i, carry):
        at = pl.ds(pl.multiple_of(i * TILE, TILE), TILE)
        down_buf[at, :] = dot(hid[:, at], rows[:, width:], ((0,), (0,))).astype(jnp.bfloat16)
        return carry

    lax.fori_loop(0, 1, units, 0)
    lax.fori_loop(1, DEVICES, return_extra, 0)
    lanes = back.shape[1]
    near = bounce.at[:, pl.ds(0, lanes)]
    away = [
        pltpu.make_async_copy(main_slot(back, 0), main_slot(near, 0), local_sem.at[0]),
        pltpu.make_async_copy(extra_slot(back, 0, edge), extra_slot(near, 0, SLOTS), local_sem.at[1]),
    ]
    kept = [
        pltpu.make_async_copy(main_slot(near, 0), main_slot(home_main, own_index), local_sem.at[0]),
        pltpu.make_async_copy(
            extra_slot(near, 0, SLOTS), extra_slot(home_extra, own_index), local_sem.at[1]
        ),
    ]
    for item in away:
        item.start()
    lax.fori_loop(1, 2 * half // TILE, units, 0)
    for item in away:
        item.wait()
    for item in kept:
        item.start()
    lax.fori_loop(0, width // TILE, columns, 0)
    grads = zip((down_buf, gate_buf, up_buf), (down_grad, gate_grad, up_grad))
    moves = []
    for i, (buf, out) in enumerate(grads):
        moves.append(remote(part(buf, 1), out.at[core], grad_send.at[i], grad_recv.at[i], partner))
        moves.append(pltpu.make_async_copy(part(buf, 0), out.at[core], load_sem.at[i]))
    for item in moves:
        item.start()

    def home_came(k, carry):
        index = half_and_expert(*target(k))
        for kind in range(2):
            home_copy(k, source(k), index, kind).wait_recv()
        return carry

    lax.fori_loop(1, DEVICES, home_came, 0)
    for item in kept:
        item.wait()

    total, score = None, None
    for pick, home, slots in ((pick_main, home_main, SLOTS), (pick_extra, home_extra, EXTRA)):
        count = experts * slots
        one_hot = pick[...]
        tail = home[:, width:].astype(high)
        tail = jnp.sum(tail[:count] + tail[count:], axis=1, keepdims=True)
        group = iota((count, experts), 0) // slots == iota((count, experts), 1)
        spread = jnp.where(group, tail, 0.0)
        spread_high = spread.astype(low)
        spread_low = (spread - spread_high.astype(high)).astype(low)
        here = dot(one_hot, spread_high, ((1,), (0,))) + dot(one_hot, spread_low, ((1,), (0,)))
        score = here if score is None else score + here
        both = dot(one_hot, home[:count, :width], ((1,), (0,)))
        both = both + dot(one_hot, home[count:, :width], ((1,), (0,)))
        total = both if total is None else total + both
    grad_logits = (
        score - gates[...] * jnp.sum(score, axis=1, keepdims=True)
    ).astype(low)
    grad_normed = total + dot(grad_logits, router_weight[...], ((1,), (0,)))
    inverse, scaled, gained = normalized()
    gain = grad_normed * scaled
    gain_high = gain.astype(low)
    gain_low = (gain - gain_high.astype(high)).astype(low)
    ones = jnp.ones((gain.shape[0], experts), low)
    gain_sum = dot(gain_high, ones, ((0,), (0,))) + dot(gain_low, ones, ((0,), (0,)))
    lane = iota(gain_sum.shape, 1)
    sum_high = gain_sum.astype(low).astype(high)
    gain_parts = jnp.where(lane == 0, sum_high, jnp.where(lane == 1, gain_sum - sum_high, 0.0))
    router_part = dot(gained, grad_logits, ((0,), (0,)))
    part = jnp.concatenate([router_part, gain_parts], axis=1).astype(low)
    part_sums[...] = part.reshape(part_sums.shape)
    grad_scaled = grad_normed * gain_row
    correction = jnp.mean(grad_scaled * scaled, axis=1, keepdims=True)
    grad_tokens[...] = (
        cotangent[...].astype(high) + inverse * (grad_scaled - scaled * correction)
    ).astype(low)

    pairs = part_sums.shape[0] // DEVICES

    def piece(k):
        dp, ctx = target(k)
        return remote(
            part_sums.at[pl.ds((dp * 32 + ctx) * pairs, pairs)], all_sums.at[k],
            sum_send.at[k], sum_recv.at[k], (dp, ctx),
        )

    def piece_go(k, carry):
        piece(k).start()
        return carry

    lax.fori_loop(1, DEVICES, piece_go, 0)
    all_sums[0] = part_sums[pl.ds((mine[0] * 32 + mine[1]) * pairs, pairs)]

    def drain(k, carry):
        go_main(k).wait_send()
        go_extra(k).wait_send()
        for kind in range(2):
            home_copy(k, source(k), own_index, kind).wait_send()
        return carry

    lax.fori_loop(1, DEVICES, drain, 0)
    for item in moves:
        item.wait()

    def piece_came(k, carry):
        piece(k).wait()
        return carry

    lax.fori_loop(1, DEVICES, piece_came, 0)
    sums[...] = jnp.sum(all_sums[...].astype(high), axis=0)


TILE = 256


def moe(weights, local):
    half, width = weights[2].shape[1:]
    units = 2 * half
    count = DEVICES * (SLOTS + EXTRA)
    low = jnp.bfloat16
    anywhere = pl.BlockSpec(memory_space=pl.ANY)
    pair = pltpu.SemaphoreType.DMA((2, DEVICES))
    three = pltpu.SemaphoreType.DMA((3,))
    each = pltpu.SemaphoreType.DMA((DEVICES,))
    vmem = pl.BlockSpec(memory_space=pltpu.VMEM)
    pairs = width // (2 * DEVICES)
    here, experts = local[0].shape[0], local[4].shape[0]
    return pl.pallas_call(
        moe_kernel,
        out_shape=[
            jax.ShapeDtypeStruct(local[0].shape, low),
            jax.ShapeDtypeStruct((2, width, half), low),
            jax.ShapeDtypeStruct((2, width, half), low),
            jax.ShapeDtypeStruct((2, half, width), low),
            jax.ShapeDtypeStruct((pairs, 2, 128), jnp.float32),
            jax.ShapeDtypeStruct((2 * SLOTS, 2 * width), low),
        ],
        in_specs=[anywhere] * 3 + [vmem] * 5,
        out_specs=[vmem] + [anywhere] * 3 + [vmem, anywhere],
        scratch_shapes=[
            pltpu.VMEM((experts * SLOTS, 2 * width), low),
            pltpu.VMEM((experts * EXTRA, 2 * width), low),
            pltpu.VMEM((here, experts * SLOTS), low),
            pltpu.VMEM((here, experts * EXTRA), low),
            pltpu.VMEM((here, experts), jnp.float32),
            pltpu.VMEM((DEVICES * SLOTS, width + 128), low),
            pltpu.VMEM((DEVICES * EXTRA, width + 128), low),
            pltpu.VMEM((DEVICES * pairs, 2, 128), low),
            pltpu.VMEM((DEVICES, pairs, 2, 128), low),
            pltpu.VMEM((count, 2 * width), low),
            pltpu.VMEM((count, width + 128), low),
            pltpu.VMEM((width, units), low),
            pltpu.VMEM((width, units), low),
            pltpu.VMEM((units, width), low),
            pltpu.VMEM((count, units), low),
            pltpu.VMEM((count, units), low),
            pltpu.VMEM((count, units), low),
            pltpu.VMEM((width, units), low),
            pltpu.VMEM((width, units), low),
            pltpu.VMEM((units, width), low),
            pair, pair, pair, pair,
            pltpu.SemaphoreType.DMA((2,)),
            three, three, three, three, three,
            each, each,
        ],
        compiler_params=pltpu.CompilerParams(
            collective_id=1, has_side_effects=True, vmem_limit_bytes=60 * 2**20
        ),
    )(*weights, *local)


def settle_kernel(*refs):
    count = (len(refs) - 2) // 3
    ins, outs, held = refs[:count], refs[count : 2 * count], refs[2 * count : 3 * count]
    in_sem, out_sem = refs[3 * count :]
    takes = [pltpu.make_async_copy(a, b, in_sem.at[i]) for i, (a, b) in enumerate(zip(ins, held))]
    gives = [pltpu.make_async_copy(a, b, out_sem.at[i]) for i, (a, b) in enumerate(zip(held, outs))]
    for item in takes:
        item.start()
    for take, give in zip(takes, gives):
        take.wait()
        give.start()
    for item in gives:
        item.wait()


def settle(arrays):
    anywhere = pl.BlockSpec(memory_space=pl.ANY)
    count = len(arrays)
    return pl.pallas_call(
        settle_kernel,
        out_shape=[jax.ShapeDtypeStruct(a.shape, a.dtype) for a in arrays],
        in_specs=[anywhere] * count,
        out_specs=[anywhere] * count,
        scratch_shapes=[pltpu.VMEM(a.shape, a.dtype) for a in arrays]
        + [pltpu.SemaphoreType.DMA((count,)), pltpu.SemaphoreType.DMA((count,))],
        compiler_params=pltpu.CompilerParams(vmem_limit_bytes=60 * 2**20),
        cost_estimate=pl.CostEstimate(flops=10**6, bytes_accessed=17 * 2**20, transcendentals=0),
    )(*arrays)


def body(
    tokens, cotangent, expert_ids, norm_gain, router_weight, gate_weight, up_weight, down_weight
):
    experts = router_weight.shape[1]
    width = tokens.shape[1]
    grad_tokens, *grads, sums, _ = moe(
        (gate_weight, up_weight, down_weight),
        (tokens, cotangent, expert_ids.T, norm_gain.reshape(width // 128, 128), router_weight.T),
    )
    sums = sums.reshape(width // DEVICES, 128)
    grad_tokens, *grads = settle([grad_tokens, *grads])
    return (grad_tokens, *grads, sums[:, :experts], sums[:, experts] + sums[:, experts + 1])


def solution(mesh):
    return jax.shard_map(
        body,
        mesh=mesh,
        in_specs=(
            P(("dp", "ctx"), None),
            P(("dp", "ctx"), None),
            P(("dp", "ctx"), None),
            P(),
            P(),
            P("ctx", None, "dp"),
            P("ctx", None, "dp"),
            P("ctx", "dp", None),
        ),
        out_specs=(
            P(("dp", "ctx"), None),
            P("ctx", None, "dp"),
            P("ctx", None, "dp"),
            P("ctx", "dp", None),
            P(("dp", "ctx"), None),
            P(("dp", "ctx")),
        ),
        check_vma=False,
    )
```

```python
import functools

import jax
import jax.numpy as jnp
from jax import lax
from jax.experimental import pallas as pl
from jax.experimental.pallas import tpu as pltpu
from jax.sharding import PartitionSpec as P

EPSILON = 1e-05
SWISH_SCALE = 1.702
MESH = pl.DeviceIdType.MESH
SLOTS = 8
EXTRA = 2
ROW_BLOCK = 256
DEVICES = 128


def coordinates():
    dp, ctx = lax.axis_index("dp"), lax.axis_index("ctx")
    return (ctx // 4) % 4, ctx % 4, (dp // 2) * 2 + ctx // 16, dp % 2


def device_of(x, y, z, core):
    return (z // 2) * 2 + core, (z % 2) * 16 + x * 4 + y


def expert_of(dp, ctx):
    return 2 * ctx + dp % 2


def half_and_expert(dp, ctx):
    return (dp // 2) * 64 + expert_of(dp, ctx)


def dot(a, b, contract):
    return lax.dot_general(a, b, (contract, ((), ())), preferred_element_type=jnp.float32)


def moe_kernel(
    gate_weight, up_weight, down_weight,
    tokens, cotangent, expert_ids, norm_gain, router_weight,
    grad_tokens, gate_grad, up_grad, down_grad, sums, bounce,
    out_main, out_extra, pick_main, pick_extra, gates, home_main, home_extra, part_sums, all_sums, rows, back, w_gate, w_up, w_down, hid, gat, upp, gate_buf, up_buf, down_buf,
    go_send, go_recv, home_send, home_recv, local_sem, load_sem,
    weight_send, weight_recv, grad_send, grad_recv, sum_send, sum_recv,
):
    x, y, z, core = coordinates()
    mine = device_of(x, y, z, core)
    partner = device_of(x, y, z, 1 - core)
    edge = DEVICES * SLOTS
    half = down_weight.shape[1]
    width = down_weight.shape[2]

    def turn(k, sign, flip):
        return device_of(
            (x + sign * (2 * k + k // 4) + 4 * DEVICES) % 4,
            (y + sign * k + 4 * DEVICES) % 4,
            (z + sign * (3 * k + k // 4 + k // 16) + 4 * DEVICES) % 4,
            flip,
        )

    def target(k):
        return turn(k, 1 - 2 * core, (core + k // 64 + k // 16) % 2)

    def source(k):
        other = (core + k // 64 + k // 16) % 2
        return turn(k, 2 * other - 1, other)

    def main_slot(ref, i):
        return ref.at[pl.ds(pl.multiple_of(i * SLOTS, SLOTS), SLOTS)]

    def extra_slot(ref, i, first=0):
        return ref.at[pl.ds(pl.multiple_of(first + i * EXTRA, EXTRA), EXTRA)]

    barrier = pltpu.get_barrier_semaphore()

    def greet(k, carry):
        pl.semaphore_signal(barrier, inc=1, device_id=target(k), device_id_type=MESH)
        return carry

    lax.fori_loop(1, DEVICES, greet, 0)

    low, high = jnp.bfloat16, jnp.float32
    experts = router_weight.shape[0]
    tokens_here = tokens.shape[0]
    places = (w_gate, w_up, w_down)

    def part(buf, i):
        at = pl.ds(i * half, half)
        return buf.at[at] if buf.shape[0] == 2 * half else buf.at[:, at]

    loads = [
        pltpu.make_async_copy(weight.at[core], part(place, 0), load_sem.at[i])
        for i, (weight, place) in enumerate(zip((gate_weight, up_weight, down_weight), places))
    ]
    for item in loads:
        item.start()

    def iota(shape, dim):
        return lax.broadcasted_iota(jnp.int32, shape, dim)

    def as_low(flag):
        return flag.astype(high).astype(low)

    gain_row = jnp.concatenate([norm_gain[i : i + 1, :] for i in range(width // 128)], axis=1)

    def normalized():
        widened = tokens[...].astype(high)
        inverse = lax.rsqrt(jnp.mean(widened * widened, axis=1, keepdims=True) + EPSILON)
        scaled = widened * inverse
        return inverse, scaled, (scaled * gain_row).astype(low)

    normed_here = normalized()[2]
    logits = dot(normed_here, router_weight[...], ((1,), (1,)))
    label = iota((experts, tokens_here), 0)
    ids = expert_ids[...]
    turned = ids[0:1] == label
    for k in range(1, ids.shape[0]):
        turned = turned | (ids[k : k + 1] == label)
    same = iota((experts, experts), 0) == iota((experts, experts), 1)
    member = dot(as_low(turned), as_low(same), ((0,), (0,))) > 0.5
    lifted = jnp.where(member, jnp.exp(jnp.where(member, logits, 0.0)), 0.0)
    gate = lifted / jnp.sum(lifted, axis=1, keepdims=True)
    gates[...] = gate
    gate_high = gate.astype(low)
    gate_low = (gate - gate_high.astype(high)).astype(low)
    earlier = iota((tokens_here, tokens_here), 0) > iota((tokens_here, tokens_here), 1)
    named = as_low(member)
    rank = dot(as_low(earlier), named, ((1,), (0,)))
    rank = jnp.where(member, rank, -1.0).astype(low)
    for out, chosen, slots, first in (
        (out_main, pick_main, SLOTS, 0), (out_extra, pick_extra, EXTRA, SLOTS)
    ):
        count = experts * slots
        spread = (iota((experts, count), 1) // slots == iota((experts, count), 0))
        spread = as_low(spread)
        slot = (iota((tokens_here, count), 1) % slots + first).astype(high)
        hit = dot(rank, spread, ((1,), (0,))) == slot
        one_hot = as_low(hit)
        chosen[...] = one_hot
        out[:, :width] = dot(one_hot, normed_here, ((0,), (0,))).astype(low)
        scaled_up = None
        for piece_of in (gate_high, gate_low):
            weighted = jnp.where(hit, dot(piece_of, spread, ((1,), (0,))), 0.0).astype(low)
            term = dot(weighted, cotangent[...], ((0,), (0,)))
            scaled_up = term if scaled_up is None else scaled_up + term
        out[:, width:] = scaled_up.astype(low)

    pl.semaphore_wait(barrier, DEVICES - 1)

    def remote(src, dst, send, recv, device):
        return pltpu.make_async_remote_copy(
            src_ref=src, dst_ref=dst, send_sem=send, recv_sem=recv,
            device_id=device, device_id_type=MESH,
        )

    def go_main(k):
        to = target(k)
        return remote(
            main_slot(out_main, expert_of(*to)), main_slot(rows, k),
            go_send.at[0, k], go_recv.at[0, k], to,
        )

    def go_extra(k):
        to = target(k)
        return remote(
            extra_slot(out_extra, expert_of(*to)), extra_slot(rows, k, edge),
            go_send.at[1, k], go_recv.at[1, k], to,
        )

    def home_copy(k, to, index, kind):
        if kind == 0:
            src, dst = main_slot(back, k), main_slot(home_main, index)
        else:
            src, dst = extra_slot(back, k, edge), extra_slot(home_extra, index)
        return remote(src, dst, home_send.at[kind, k], home_recv.at[kind, index], to)

    own_index = half_and_expert(*mine)

    def return_main(k, carry):
        home_copy(k, source(k), own_index, 0).start()
        return carry

    def return_extra(k, carry):
        home_copy(k, source(k), own_index, 1).start()
        return carry

    swaps = [
        remote(weight.at[1 - core], part(place, 1), weight_send.at[i], weight_recv.at[i], partner)
        for i, (weight, place) in enumerate(zip((gate_weight, up_weight, down_weight), places))
    ]
    own = expert_of(*mine)
    leave = [
        pltpu.make_async_copy(main_slot(out_main, own), main_slot(bounce, 0), local_sem.at[0]),
        pltpu.make_async_copy(extra_slot(out_extra, own), extra_slot(bounce, 0, SLOTS), local_sem.at[1]),
    ]
    enter = [
        pltpu.make_async_copy(main_slot(bounce, 0), main_slot(rows, 0), local_sem.at[0]),
        pltpu.make_async_copy(
            extra_slot(bounce, 0, SLOTS), extra_slot(rows, 0, edge), local_sem.at[1]
        ),
    ]

    def go(k, carry):
        go_main(k).start()
        go_extra(k).start()
        return carry

    lax.fori_loop(1, DEVICES, go, 0)
    for item in swaps + leave:
        item.start()
    for item in leave:
        item.wait()
    for item in enter:
        item.start()
    for item in loads + swaps + enter:
        item.wait()

    def main_came(k, carry):
        go_main(k).wait_recv()
        return carry

    def extra_came(k, carry):
        go_extra(k).wait_recv()
        return carry

    senders = ROW_BLOCK // SLOTS
    blocks = edge // ROW_BLOCK

    def step(i, carry):
        first = i * senders
        lax.fori_loop(jnp.maximum(first, 1), jnp.minimum(first + senders, DEVICES), main_came, 0)
        lax.fori_loop(DEVICES - (i // blocks) * (DEVICES - 1), DEVICES, extra_came, 0)
        block = pl.ds(pl.multiple_of(i * ROW_BLOCK, ROW_BLOCK), ROW_BLOCK)
        normed = rows[block, :width]
        upstream = rows[block, width:]
        gate_pre = dot(normed, w_gate[...], ((1,), (0,)))
        up_pre = dot(normed, w_up[...], ((1,), (0,))) + 1.0
        grad_hidden = dot(upstream, w_down[...], ((1,), (1,)))
        squash = jax.nn.sigmoid(SWISH_SCALE * gate_pre)
        swish = gate_pre * squash
        hidden = (swish * up_pre).astype(jnp.bfloat16)
        slope = squash + SWISH_SCALE * swish * (1.0 - squash)
        pre_gate = (grad_hidden * up_pre * slope).astype(jnp.bfloat16)
        pre_up = (grad_hidden * swish).astype(jnp.bfloat16)
        hid[block, :] = hidden
        gat[block, :] = pre_gate
        upp[block, :] = pre_up
        score = jnp.sum(grad_hidden * hidden.astype(jnp.float32), axis=1, keepdims=True)
        high = score.astype(jnp.bfloat16).astype(jnp.float32)
        lane = lax.broadcasted_iota(jnp.int32, (ROW_BLOCK, 128), 1)
        tail = jnp.where(lane == 0, high, jnp.where(lane == 1, score - high, 0.0))
        total = dot(pre_gate, w_gate[...], ((1,), (1,))) + dot(pre_up, w_up[...], ((1,), (1,)))
        back[block, :width] = total.astype(jnp.bfloat16)
        back[block, width:] = tail.astype(jnp.bfloat16)
        lax.fori_loop(jnp.maximum(first - senders, 1), first, return_main, 0)
        return carry

    lax.fori_loop(0, blocks + 1, step, 0)

    def columns(i, carry):
        at = pl.ds(pl.multiple_of(i * TILE, TILE), TILE)
        tile = rows[:, at]
        gate_buf[at, :] = dot(tile, gat[...], ((0,), (0,))).astype(jnp.bfloat16)
        up_buf[at, :] = dot(tile, upp[...], ((0,), (0,))).astype(jnp.bfloat16)
        return carry

    def units(i, carry):
        at = pl.ds(pl.multiple_of(i * TILE, TILE), TILE)
        down_buf[at, :] = dot(hid[:, at], rows[:, width:], ((0,), (0,))).astype(jnp.bfloat16)
        return carry

    lax.fori_loop(0, 1, units, 0)
    lax.fori_loop(1, DEVICES, return_extra, 0)
    lanes = back.shape[1]
    near = bounce.at[:, pl.ds(0, lanes)]
    away = [
        pltpu.make_async_copy(main_slot(back, 0), main_slot(near, 0), local_sem.at[0]),
        pltpu.make_async_copy(extra_slot(back, 0, edge), extra_slot(near, 0, SLOTS), local_sem.at[1]),
    ]
    kept = [
        pltpu.make_async_copy(main_slot(near, 0), main_slot(home_main, own_index), local_sem.at[0]),
        pltpu.make_async_copy(
            extra_slot(near, 0, SLOTS), extra_slot(home_extra, own_index), local_sem.at[1]
        ),
    ]
    for item in away:
        item.start()
    lax.fori_loop(1, 2 * half // TILE, units, 0)
    for item in away:
        item.wait()
    for item in kept:
        item.start()
    lax.fori_loop(0, width // TILE, columns, 0)
    grads = zip((down_buf, gate_buf, up_buf), (down_grad, gate_grad, up_grad))
    moves = []
    for i, (buf, out) in enumerate(grads):
        moves.append(remote(part(buf, 1), out.at[core], grad_send.at[i], grad_recv.at[i], partner))
        moves.append(pltpu.make_async_copy(part(buf, 0), out.at[core], load_sem.at[i]))
    for item in moves:
        item.start()

    def home_came(k, carry):
        index = half_and_expert(*target(k))
        for kind in range(2):
            home_copy(k, source(k), index, kind).wait_recv()
        return carry

    lax.fori_loop(1, DEVICES, home_came, 0)
    for item in kept:
        item.wait()

    total, score = None, None
    for pick, home, slots in ((pick_main, home_main, SLOTS), (pick_extra, home_extra, EXTRA)):
        count = experts * slots
        one_hot = pick[...]
        tail = home[:, width:].astype(high)
        tail = jnp.sum(tail[:count] + tail[count:], axis=1, keepdims=True)
        group = iota((count, experts), 0) // slots == iota((count, experts), 1)
        spread = jnp.where(group, tail, 0.0)
        spread_high = spread.astype(low)
        spread_low = (spread - spread_high.astype(high)).astype(low)
        here = dot(one_hot, spread_high, ((1,), (0,))) + dot(one_hot, spread_low, ((1,), (0,)))
        score = here if score is None else score + here
        both = dot(one_hot, home[:count, :width], ((1,), (0,)))
        both = both + dot(one_hot, home[count:, :width], ((1,), (0,)))
        total = both if total is None else total + both
    grad_logits = (
        score - gates[...] * jnp.sum(score, axis=1, keepdims=True)
    ).astype(low)
    grad_normed = total + dot(grad_logits, router_weight[...], ((1,), (0,)))
    inverse, scaled, gained = normalized()
    gain = grad_normed * scaled
    gain_high = gain.astype(low)
    gain_low = (gain - gain_high.astype(high)).astype(low)
    ones = jnp.ones((gain.shape[0], experts), low)
    gain_sum = dot(gain_high, ones, ((0,), (0,))) + dot(gain_low, ones, ((0,), (0,)))
    lane = iota(gain_sum.shape, 1)
    sum_high = gain_sum.astype(low).astype(high)
    gain_parts = jnp.where(lane == 0, sum_high, jnp.where(lane == 1, gain_sum - sum_high, 0.0))
    router_part = dot(gained, grad_logits, ((0,), (0,)))
    part = jnp.concatenate([router_part, gain_parts], axis=1).astype(low)
    part_sums[...] = part.reshape(part_sums.shape)
    grad_scaled = grad_normed * gain_row
    correction = jnp.mean(grad_scaled * scaled, axis=1, keepdims=True)
    grad_tokens[...] = (
        cotangent[...].astype(high) + inverse * (grad_scaled - scaled * correction)
    ).astype(low)

    pairs = part_sums.shape[0] // DEVICES

    def piece(k):
        dp, ctx = target(k)
        return remote(
            part_sums.at[pl.ds((dp * 32 + ctx) * pairs, pairs)], all_sums.at[k],
            sum_send.at[k], sum_recv.at[k], (dp, ctx),
        )

    def piece_go(k, carry):
        piece(k).start()
        return carry

    lax.fori_loop(1, DEVICES, piece_go, 0)
    all_sums[0] = part_sums[pl.ds((mine[0] * 32 + mine[1]) * pairs, pairs)]

    def drain(k, carry):
        go_main(k).wait_send()
        go_extra(k).wait_send()
        for kind in range(2):
            home_copy(k, source(k), own_index, kind).wait_send()
        return carry

    lax.fori_loop(1, DEVICES, drain, 0)
    for item in moves:
        item.wait()

    def piece_came(k, carry):
        piece(k).wait()
        return carry

    lax.fori_loop(1, DEVICES, piece_came, 0)
    sums[...] = jnp.sum(all_sums[...].astype(high), axis=0)


TILE = 256


def moe(weights, local):
    half, width = weights[2].shape[1:]
    units = 2 * half
    count = DEVICES * (SLOTS + EXTRA)
    low = jnp.bfloat16
    anywhere = pl.BlockSpec(memory_space=pl.ANY)
    pair = pltpu.SemaphoreType.DMA((2, DEVICES))
    three = pltpu.SemaphoreType.DMA((3,))
    each = pltpu.SemaphoreType.DMA((DEVICES,))
    vmem = pl.BlockSpec(memory_space=pltpu.VMEM)
    pairs = width // (2 * DEVICES)
    here, experts = local[0].shape[0], local[4].shape[0]
    return pl.pallas_call(
        moe_kernel,
        out_shape=[
            jax.ShapeDtypeStruct(local[0].shape, low),
            jax.ShapeDtypeStruct((2, width, half), low),
            jax.ShapeDtypeStruct((2, width, half), low),
            jax.ShapeDtypeStruct((2, half, width), low),
            jax.ShapeDtypeStruct((pairs, 2, 128), jnp.float32),
            jax.ShapeDtypeStruct((2 * SLOTS, 2 * width), low),
        ],
        in_specs=[anywhere] * 3 + [vmem] * 5,
        out_specs=[vmem] + [anywhere] * 3 + [vmem, anywhere],
        scratch_shapes=[
            pltpu.VMEM((experts * SLOTS, 2 * width), low),
            pltpu.VMEM((experts * EXTRA, 2 * width), low),
            pltpu.VMEM((here, experts * SLOTS), low),
            pltpu.VMEM((here, experts * EXTRA), low),
            pltpu.VMEM((here, experts), jnp.float32),
            pltpu.VMEM((DEVICES * SLOTS, width + 128), low),
            pltpu.VMEM((DEVICES * EXTRA, width + 128), low),
            pltpu.VMEM((DEVICES * pairs, 2, 128), low),
            pltpu.VMEM((DEVICES, pairs, 2, 128), low),
            pltpu.VMEM((count, 2 * width), low),
            pltpu.VMEM((count, width + 128), low),
            pltpu.VMEM((width, units), low),
            pltpu.VMEM((width, units), low),
            pltpu.VMEM((units, width), low),
            pltpu.VMEM((count, units), low),
            pltpu.VMEM((count, units), low),
            pltpu.VMEM((count, units), low),
            pltpu.VMEM((width, units), low),
            pltpu.VMEM((width, units), low),
            pltpu.VMEM((units, width), low),
            pair, pair, pair, pair,
            pltpu.SemaphoreType.DMA((2,)),
            three, three, three, three, three,
            each, each,
        ],
        compiler_params=pltpu.CompilerParams(
            collective_id=1, has_side_effects=True, vmem_limit_bytes=60 * 2**20
        ),
    )(*weights, *local)


def settle_kernel(*refs):
    count = (len(refs) - 2) // 3
    ins, outs, held = refs[:count], refs[count : 2 * count], refs[2 * count : 3 * count]
    in_sem, out_sem = refs[3 * count :]
    takes = [pltpu.make_async_copy(a, b, in_sem.at[i]) for i, (a, b) in enumerate(zip(ins, held))]
    gives = [pltpu.make_async_copy(a, b, out_sem.at[i]) for i, (a, b) in enumerate(zip(held, outs))]
    for item in takes:
        item.start()
    for take, give in zip(takes, gives):
        take.wait()
        give.start()
    for item in gives:
        item.wait()


def settle(arrays):
    anywhere = pl.BlockSpec(memory_space=pl.ANY)
    count = len(arrays)
    return pl.pallas_call(
        settle_kernel,
        out_shape=[jax.ShapeDtypeStruct(a.shape, a.dtype) for a in arrays],
        in_specs=[anywhere] * count,
        out_specs=[anywhere] * count,
        scratch_shapes=[pltpu.VMEM(a.shape, a.dtype) for a in arrays]
        + [pltpu.SemaphoreType.DMA((count,)), pltpu.SemaphoreType.DMA((count,))],
        compiler_params=pltpu.CompilerParams(vmem_limit_bytes=60 * 2**20),
        cost_estimate=pl.CostEstimate(flops=10**6, bytes_accessed=17 * 2**20, transcendentals=0),
    )(*arrays)


def body(
    tokens, cotangent, expert_ids, norm_gain, router_weight, gate_weight, up_weight, down_weight
):
    experts = router_weight.shape[1]
    width = tokens.shape[1]
    grad_tokens, *grads, sums, _ = moe(
        (gate_weight, up_weight, down_weight),
        (tokens, cotangent, expert_ids.T, norm_gain.reshape(width // 128, 128), router_weight.T),
    )
    sums = sums.reshape(width // DEVICES, 128)
    grad_tokens, *grads = settle([grad_tokens, *grads])
    return (grad_tokens, *grads, sums[:, :experts], sums[:, experts] + sums[:, experts + 1])


def solution(mesh):
    return jax.shard_map(
        body,
        mesh=mesh,
        in_specs=(
            P(("dp", "ctx"), None),
            P(("dp", "ctx"), None),
            P(("dp", "ctx"), None),
            P(),
            P(),
            P("ctx", None, "dp"),
            P("ctx", None, "dp"),
            P("ctx", "dp", None),
        ),
        out_specs=(
            P(("dp", "ctx"), None),
            P("ctx", None, "dp"),
            P("ctx", None, "dp"),
            P("ctx", "dp", None),
            P(("dp", "ctx"), None),
            P(("dp", "ctx")),
        ),
        check_vma=False,
    )
```

```python
import functools

import jax
import jax.numpy as jnp
from jax import lax
from jax.experimental import pallas as pl
from jax.experimental.pallas import tpu as pltpu
from jax.sharding import PartitionSpec as P

EPSILON = 1e-05
SWISH_SCALE = 1.702
MESH = pl.DeviceIdType.MESH
SLOTS = 8
EXTRA = 2
ROW_BLOCK = 256
DEVICES = 128


def coordinates():
    dp, ctx = lax.axis_index("dp"), lax.axis_index("ctx")
    return (ctx // 4) % 4, ctx % 4, (dp // 2) * 2 + ctx // 16, dp % 2


def device_of(x, y, z, core):
    return (z // 2) * 2 + core, (z % 2) * 16 + x * 4 + y


def expert_of(dp, ctx):
    return 2 * ctx + dp % 2


def half_and_expert(dp, ctx):
    return (dp // 2) * 64 + expert_of(dp, ctx)


def dot(a, b, contract):
    return lax.dot_general(a, b, (contract, ((), ())), preferred_element_type=jnp.float32)


def moe_kernel(
    gate_weight, up_weight, down_weight,
    tokens, cotangent, expert_ids, norm_gain, router_weight,
    grad_tokens, gate_grad, up_grad, down_grad, sums, bounce,
    out_main, out_extra, pick_main, pick_extra, gates, home_main, home_extra, part_sums, all_sums, rows, back, w_gate, w_up, w_down, hid, gat, upp, gate_buf, up_buf, down_buf,
    go_send, go_recv, home_send, home_recv, local_sem, load_sem,
    weight_send, weight_recv, grad_send, grad_recv, sum_send, sum_recv,
):
    x, y, z, core = coordinates()
    mine = device_of(x, y, z, core)
    partner = device_of(x, y, z, 1 - core)
    edge = DEVICES * SLOTS
    half = down_weight.shape[1]
    width = down_weight.shape[2]

    def turn(k, sign, flip):
        return device_of(
            (x + sign * (2 * k + k // 4) + 4 * DEVICES) % 4,
            (y - sign * k + 4 * DEVICES) % 4,
            (z + sign * (3 * k + k // 4 + k // 16) + 4 * DEVICES) % 4,
            flip,
        )

    def target(k):
        return turn(k, 1 - 2 * core, (core + k // 64 + k // 16) % 2)

    def source(k):
        other = (core + k // 64 + k // 16) % 2
        return turn(k, 2 * other - 1, other)

    def main_slot(ref, i):
        return ref.at[pl.ds(pl.multiple_of(i * SLOTS, SLOTS), SLOTS)]

    def extra_slot(ref, i, first=0):
        return ref.at[pl.ds(pl.multiple_of(first + i * EXTRA, EXTRA), EXTRA)]

    barrier = pltpu.get_barrier_semaphore()

    def greet(k, carry):
        pl.semaphore_signal(barrier, inc=1, device_id=target(k), device_id_type=MESH)
        return carry

    lax.fori_loop(1, DEVICES, greet, 0)

    low, high = jnp.bfloat16, jnp.float32
    experts = router_weight.shape[0]
    tokens_here = tokens.shape[0]
    places = (w_gate, w_up, w_down)

    def part(buf, i):
        at = pl.ds(i * half, half)
        return buf.at[at] if buf.shape[0] == 2 * half else buf.at[:, at]

    loads = [
        pltpu.make_async_copy(weight.at[core], part(place, 0), load_sem.at[i])
        for i, (weight, place) in enumerate(zip((gate_weight, up_weight, down_weight), places))
    ]
    for item in loads:
        item.start()

    def iota(shape, dim):
        return lax.broadcasted_iota(jnp.int32, shape, dim)

    def as_low(flag):
        return flag.astype(high).astype(low)

    gain_row = jnp.concatenate([norm_gain[i : i + 1, :] for i in range(width // 128)], axis=1)

    def normalized():
        widened = tokens[...].astype(high)
        inverse = lax.rsqrt(jnp.mean(widened * widened, axis=1, keepdims=True) + EPSILON)
        scaled = widened * inverse
        return inverse, scaled, (scaled * gain_row).astype(low)

    normed_here = normalized()[2]
    logits = dot(normed_here, router_weight[...], ((1,), (1,)))
    label = iota((experts, tokens_here), 0)
    ids = expert_ids[...]
    turned = ids[0:1] == label
    for k in range(1, ids.shape[0]):
        turned = turned | (ids[k : k + 1] == label)
    same = iota((experts, experts), 0) == iota((experts, experts), 1)
    member = dot(as_low(turned), as_low(same), ((0,), (0,))) > 0.5
    lifted = jnp.where(member, jnp.exp(jnp.where(member, logits, 0.0)), 0.0)
    gate = lifted / jnp.sum(lifted, axis=1, keepdims=True)
    gates[...] = gate
    gate_high = gate.astype(low)
    gate_low = (gate - gate_high.astype(high)).astype(low)
    earlier = iota((tokens_here, tokens_here), 0) > iota((tokens_here, tokens_here), 1)
    named = as_low(member)
    rank = dot(as_low(earlier), named, ((1,), (0,)))
    rank = jnp.where(member, rank, -1.0).astype(low)
    for out, chosen, slots, first in (
        (out_main, pick_main, SLOTS, 0), (out_extra, pick_extra, EXTRA, SLOTS)
    ):
        count = experts * slots
        spread = (iota((experts, count), 1) // slots == iota((experts, count), 0))
        spread = as_low(spread)
        slot = (iota((tokens_here, count), 1) % slots + first).astype(high)
        hit = dot(rank, spread, ((1,), (0,))) == slot
        one_hot = as_low(hit)
        chosen[...] = one_hot
        out[:, :width] = dot(one_hot, normed_here, ((0,), (0,))).astype(low)
        scaled_up = None
        for piece_of in (gate_high, gate_low):
            weighted = jnp.where(hit, dot(piece_of, spread, ((1,), (0,))), 0.0).astype(low)
            term = dot(weighted, cotangent[...], ((0,), (0,)))
            scaled_up = term if scaled_up is None else scaled_up + term
        out[:, width:] = scaled_up.astype(low)

    pl.semaphore_wait(barrier, DEVICES - 1)

    def remote(src, dst, send, recv, device):
        return pltpu.make_async_remote_copy(
            src_ref=src, dst_ref=dst, send_sem=send, recv_sem=recv,
            device_id=device, device_id_type=MESH,
        )

    def go_main(k):
        to = target(k)
        return remote(
            main_slot(out_main, expert_of(*to)), main_slot(rows, k),
            go_send.at[0, k], go_recv.at[0, k], to,
        )

    def go_extra(k):
        to = target(k)
        return remote(
            extra_slot(out_extra, expert_of(*to)), extra_slot(rows, k, edge),
            go_send.at[1, k], go_recv.at[1, k], to,
        )

    def home_copy(k, to, index, kind):
        if kind == 0:
            src, dst = main_slot(back, k), main_slot(home_main, index)
        else:
            src, dst = extra_slot(back, k, edge), extra_slot(home_extra, index)
        return remote(src, dst, home_send.at[kind, k], home_recv.at[kind, index], to)

    own_index = half_and_expert(*mine)

    def return_main(k, carry):
        home_copy(k, source(k), own_index, 0).start()
        return carry

    def return_extra(k, carry):
        home_copy(k, source(k), own_index, 1).start()
        return carry

    swaps = [
        remote(weight.at[1 - core], part(place, 1), weight_send.at[i], weight_recv.at[i], partner)
        for i, (weight, place) in enumerate(zip((gate_weight, up_weight, down_weight), places))
    ]
    own = expert_of(*mine)
    leave = [
        pltpu.make_async_copy(main_slot(out_main, own), main_slot(bounce, 0), local_sem.at[0]),
        pltpu.make_async_copy(extra_slot(out_extra, own), extra_slot(bounce, 0, SLOTS), local_sem.at[1]),
    ]
    enter = [
        pltpu.make_async_copy(main_slot(bounce, 0), main_slot(rows, 0), local_sem.at[0]),
        pltpu.make_async_copy(
            extra_slot(bounce, 0, SLOTS), extra_slot(rows, 0, edge), local_sem.at[1]
        ),
    ]

    def go(k, carry):
        go_main(k).start()
        go_extra(k).start()
        return carry

    lax.fori_loop(1, DEVICES, go, 0)
    for item in swaps + leave:
        item.start()
    for item in leave:
        item.wait()
    for item in enter:
        item.start()
    for item in loads + swaps + enter:
        item.wait()

    def main_came(k, carry):
        go_main(k).wait_recv()
        return carry

    def extra_came(k, carry):
        go_extra(k).wait_recv()
        return carry

    senders = ROW_BLOCK // SLOTS
    blocks = edge // ROW_BLOCK

    def step(i, carry):
        first = i * senders
        lax.fori_loop(jnp.maximum(first, 1), jnp.minimum(first + senders, DEVICES), main_came, 0)
        lax.fori_loop(DEVICES - (i // blocks) * (DEVICES - 1), DEVICES, extra_came, 0)
        block = pl.ds(pl.multiple_of(i * ROW_BLOCK, ROW_BLOCK), ROW_BLOCK)
        normed = rows[block, :width]
        upstream = rows[block, width:]
        gate_pre = dot(normed, w_gate[...], ((1,), (0,)))
        up_pre = dot(normed, w_up[...], ((1,), (0,))) + 1.0
        grad_hidden = dot(upstream, w_down[...], ((1,), (1,)))
        squash = jax.nn.sigmoid(SWISH_SCALE * gate_pre)
        swish = gate_pre * squash
        hidden = (swish * up_pre).astype(jnp.bfloat16)
        slope = squash + SWISH_SCALE * swish * (1.0 - squash)
        pre_gate = (grad_hidden * up_pre * slope).astype(jnp.bfloat16)
        pre_up = (grad_hidden * swish).astype(jnp.bfloat16)
        hid[block, :] = hidden
        gat[block, :] = pre_gate
        upp[block, :] = pre_up
        score = jnp.sum(grad_hidden * hidden.astype(jnp.float32), axis=1, keepdims=True)
        high = score.astype(jnp.bfloat16).astype(jnp.float32)
        lane = lax.broadcasted_iota(jnp.int32, (ROW_BLOCK, 128), 1)
        tail = jnp.where(lane == 0, high, jnp.where(lane == 1, score - high, 0.0))
        total = dot(pre_gate, w_gate[...], ((1,), (1,))) + dot(pre_up, w_up[...], ((1,), (1,)))
        back[block, :width] = total.astype(jnp.bfloat16)
        back[block, width:] = tail.astype(jnp.bfloat16)
        lax.fori_loop(jnp.maximum(first - senders, 1), first, return_main, 0)
        return carry

    lax.fori_loop(0, blocks + 1, step, 0)

    def columns(i, carry):
        at = pl.ds(pl.multiple_of(i * TILE, TILE), TILE)
        tile = rows[:, at]
        gate_buf[at, :] = dot(tile, gat[...], ((0,), (0,))).astype(jnp.bfloat16)
        up_buf[at, :] = dot(tile, upp[...], ((0,), (0,))).astype(jnp.bfloat16)
        return carry

    def units(i, carry):
        at = pl.ds(pl.multiple_of(i * TILE, TILE), TILE)
        down_buf[at, :] = dot(hid[:, at], rows[:, width:], ((0,), (0,))).astype(jnp.bfloat16)
        return carry

    lax.fori_loop(0, 1, units, 0)
    lax.fori_loop(1, DEVICES, return_extra, 0)
    lanes = back.shape[1]
    near = bounce.at[:, pl.ds(0, lanes)]
    away = [
        pltpu.make_async_copy(main_slot(back, 0), main_slot(near, 0), local_sem.at[0]),
        pltpu.make_async_copy(extra_slot(back, 0, edge), extra_slot(near, 0, SLOTS), local_sem.at[1]),
    ]
    kept = [
        pltpu.make_async_copy(main_slot(near, 0), main_slot(home_main, own_index), local_sem.at[0]),
        pltpu.make_async_copy(
            extra_slot(near, 0, SLOTS), extra_slot(home_extra, own_index), local_sem.at[1]
        ),
    ]
    for item in away:
        item.start()
    lax.fori_loop(1, 2 * half // TILE, units, 0)
    for item in away:
        item.wait()
    for item in kept:
        item.start()
    lax.fori_loop(0, width // TILE, columns, 0)
    grads = zip((down_buf, gate_buf, up_buf), (down_grad, gate_grad, up_grad))
    moves = []
    for i, (buf, out) in enumerate(grads):
        moves.append(remote(part(buf, 1), out.at[core], grad_send.at[i], grad_recv.at[i], partner))
        moves.append(pltpu.make_async_copy(part(buf, 0), out.at[core], load_sem.at[i]))
    for item in moves:
        item.start()

    def home_came(k, carry):
        index = half_and_expert(*target(k))
        for kind in range(2):
            home_copy(k, source(k), index, kind).wait_recv()
        return carry

    lax.fori_loop(1, DEVICES, home_came, 0)
    for item in kept:
        item.wait()

    total, score = None, None
    for pick, home, slots in ((pick_main, home_main, SLOTS), (pick_extra, home_extra, EXTRA)):
        count = experts * slots
        one_hot = pick[...]
        tail = home[:, width:].astype(high)
        tail = jnp.sum(tail[:count] + tail[count:], axis=1, keepdims=True)
        group = iota((count, experts), 0) // slots == iota((count, experts), 1)
        spread = jnp.where(group, tail, 0.0)
        spread_high = spread.astype(low)
        spread_low = (spread - spread_high.astype(high)).astype(low)
        here = dot(one_hot, spread_high, ((1,), (0,))) + dot(one_hot, spread_low, ((1,), (0,)))
        score = here if score is None else score + here
        both = dot(one_hot, home[:count, :width], ((1,), (0,)))
        both = both + dot(one_hot, home[count:, :width], ((1,), (0,)))
        total = both if total is None else total + both
    grad_logits = (
        score - gates[...] * jnp.sum(score, axis=1, keepdims=True)
    ).astype(low)
    grad_normed = total + dot(grad_logits, router_weight[...], ((1,), (0,)))
    inverse, scaled, gained = normalized()
    gain = grad_normed * scaled
    gain_high = gain.astype(low)
    gain_low = (gain - gain_high.astype(high)).astype(low)
    ones = jnp.ones((gain.shape[0], experts), low)
    gain_sum = dot(gain_high, ones, ((0,), (0,))) + dot(gain_low, ones, ((0,), (0,)))
    lane = iota(gain_sum.shape, 1)
    sum_high = gain_sum.astype(low).astype(high)
    gain_parts = jnp.where(lane == 0, sum_high, jnp.where(lane == 1, gain_sum - sum_high, 0.0))
    router_part = dot(gained, grad_logits, ((0,), (0,)))
    part = jnp.concatenate([router_part, gain_parts], axis=1).astype(low)
    part_sums[...] = part.reshape(part_sums.shape)
    grad_scaled = grad_normed * gain_row
    correction = jnp.mean(grad_scaled * scaled, axis=1, keepdims=True)
    grad_tokens[...] = (
        cotangent[...].astype(high) + inverse * (grad_scaled - scaled * correction)
    ).astype(low)

    pairs = part_sums.shape[0] // DEVICES

    def piece(k):
        dp, ctx = target(k)
        return remote(
            part_sums.at[pl.ds((dp * 32 + ctx) * pairs, pairs)], all_sums.at[k],
            sum_send.at[k], sum_recv.at[k], (dp, ctx),
        )

    def piece_go(k, carry):
        piece(k).start()
        return carry

    lax.fori_loop(1, DEVICES, piece_go, 0)
    all_sums[0] = part_sums[pl.ds((mine[0] * 32 + mine[1]) * pairs, pairs)]

    def drain(k, carry):
        go_main(k).wait_send()
        go_extra(k).wait_send()
        for kind in range(2):
            home_copy(k, source(k), own_index, kind).wait_send()
        return carry

    lax.fori_loop(1, DEVICES, drain, 0)
    for item in moves:
        item.wait()

    def piece_came(k, carry):
        piece(k).wait()
        return carry

    lax.fori_loop(1, DEVICES, piece_came, 0)
    sums[...] = jnp.sum(all_sums[...].astype(high), axis=0)


TILE = 256


def moe(weights, local):
    half, width = weights[2].shape[1:]
    units = 2 * half
    count = DEVICES * (SLOTS + EXTRA)
    low = jnp.bfloat16
    anywhere = pl.BlockSpec(memory_space=pl.ANY)
    pair = pltpu.SemaphoreType.DMA((2, DEVICES))
    three = pltpu.SemaphoreType.DMA((3,))
    each = pltpu.SemaphoreType.DMA((DEVICES,))
    vmem = pl.BlockSpec(memory_space=pltpu.VMEM)
    pairs = width // (2 * DEVICES)
    here, experts = local[0].shape[0], local[4].shape[0]
    return pl.pallas_call(
        moe_kernel,
        out_shape=[
            jax.ShapeDtypeStruct(local[0].shape, low),
            jax.ShapeDtypeStruct((2, width, half), low),
            jax.ShapeDtypeStruct((2, width, half), low),
            jax.ShapeDtypeStruct((2, half, width), low),
            jax.ShapeDtypeStruct((pairs, 2, 128), jnp.float32),
            jax.ShapeDtypeStruct((2 * SLOTS, 2 * width), low),
        ],
        in_specs=[anywhere] * 3 + [vmem] * 5,
        out_specs=[vmem] + [anywhere] * 3 + [vmem, anywhere],
        scratch_shapes=[
            pltpu.VMEM((experts * SLOTS, 2 * width), low),
            pltpu.VMEM((experts * EXTRA, 2 * width), low),
            pltpu.VMEM((here, experts * SLOTS), low),
            pltpu.VMEM((here, experts * EXTRA), low),
            pltpu.VMEM((here, experts), jnp.float32),
            pltpu.VMEM((DEVICES * SLOTS, width + 128), low),
            pltpu.VMEM((DEVICES * EXTRA, width + 128), low),
            pltpu.VMEM((DEVICES * pairs, 2, 128), low),
            pltpu.VMEM((DEVICES, pairs, 2, 128), low),
            pltpu.VMEM((count, 2 * width), low),
            pltpu.VMEM((count, width + 128), low),
            pltpu.VMEM((width, units), low),
            pltpu.VMEM((width, units), low),
            pltpu.VMEM((units, width), low),
            pltpu.VMEM((count, units), low),
            pltpu.VMEM((count, units), low),
            pltpu.VMEM((count, units), low),
            pltpu.VMEM((width, units), low),
            pltpu.VMEM((width, units), low),
            pltpu.VMEM((units, width), low),
            pair, pair, pair, pair,
            pltpu.SemaphoreType.DMA((2,)),
            three, three, three, three, three,
            each, each,
        ],
        compiler_params=pltpu.CompilerParams(
            collective_id=1, has_side_effects=True, vmem_limit_bytes=60 * 2**20
        ),
    )(*weights, *local)


def settle_kernel(*refs):
    count = (len(refs) - 2) // 3
    ins, outs, held = refs[:count], refs[count : 2 * count], refs[2 * count : 3 * count]
    in_sem, out_sem = refs[3 * count :]
    takes = [pltpu.make_async_copy(a, b, in_sem.at[i]) for i, (a, b) in enumerate(zip(ins, held))]
    gives = [pltpu.make_async_copy(a, b, out_sem.at[i]) for i, (a, b) in enumerate(zip(held, outs))]
    for item in takes:
        item.start()
    for take, give in zip(takes, gives):
        take.wait()
        give.start()
    for item in gives:
        item.wait()


def settle(arrays):
    anywhere = pl.BlockSpec(memory_space=pl.ANY)
    count = len(arrays)
    return pl.pallas_call(
        settle_kernel,
        out_shape=[jax.ShapeDtypeStruct(a.shape, a.dtype) for a in arrays],
        in_specs=[anywhere] * count,
        out_specs=[anywhere] * count,
        scratch_shapes=[pltpu.VMEM(a.shape, a.dtype) for a in arrays]
        + [pltpu.SemaphoreType.DMA((count,)), pltpu.SemaphoreType.DMA((count,))],
        compiler_params=pltpu.CompilerParams(vmem_limit_bytes=60 * 2**20),
        cost_estimate=pl.CostEstimate(flops=10**6, bytes_accessed=17 * 2**20, transcendentals=0),
    )(*arrays)


def body(
    tokens, cotangent, expert_ids, norm_gain, router_weight, gate_weight, up_weight, down_weight
):
    experts = router_weight.shape[1]
    width = tokens.shape[1]
    grad_tokens, *grads, sums, _ = moe(
        (gate_weight, up_weight, down_weight),
        (tokens, cotangent, expert_ids.T, norm_gain.reshape(width // 128, 128), router_weight.T),
    )
    sums = sums.reshape(width // DEVICES, 128)
    grad_tokens, *grads = settle([grad_tokens, *grads])
    return (grad_tokens, *grads, sums[:, :experts], sums[:, experts] + sums[:, experts + 1])


def solution(mesh):
    return jax.shard_map(
        body,
        mesh=mesh,
        in_specs=(
            P(("dp", "ctx"), None),
            P(("dp", "ctx"), None),
            P(("dp", "ctx"), None),
            P(),
            P(),
            P("ctx", None, "dp"),
            P("ctx", None, "dp"),
            P("ctx", "dp", None),
        ),
        out_specs=(
            P(("dp", "ctx"), None),
            P("ctx", None, "dp"),
            P("ctx", None, "dp"),
            P("ctx", "dp", None),
            P(("dp", "ctx"), None),
            P(("dp", "ctx")),
        ),
        check_vma=False,
    )
```
